256 devices in a mesh: row: 4 (over x), col: 16 (over z, core), depth: 4 (over y).
Axes of the slice: x: 4, y: 4, z: 8, core: 2. Of those that a mesh axis runs over, the one named last changes fastest.
Arguments:
- a_cols: float32 [32768, 1024], P(('row', 'col')), may hold values from -16 to 24, as said below
- past_panels: float32 [32768, 2048], P(('row', 'col'), 'depth'), may hold values from -1 to 1
Outputs:
- factor: float32 [32768, 1024], P(('row', 'col'))
The draws below stay inside these ranges and needn't reach their ends.
Inputs may be any that keep to these rules, and one draw needn't show every extreme that they name: a_cols minus past_panels times the transpose of the top 1024 rows of past_panels is the first 1024 columns of a symmetric positive definite matrix whose top block has eigenvalues between 2 and 12.
All inputs are finite; a program needn't handle non-finite values.
Results may differ from the reference program's by a relative error of at most 0.0001.
Values sent between devices are 32-bit elements.
A program may use at most 64 MiB of HBM per device.

```python
import math
import jax
import jax.numpy as jnp
from jax import lax

NB = 512
STEPS = 2
ROWS = 32768
W = 1024
PAST = 2048


def shared_draw(key):
    spread = jnp.sqrt(jnp.float32(0.4) / PAST)
    past = jnp.clip(jax.random.normal(jax.random.fold_in(key, 11), (ROWS, PAST), jnp.float32), -5.0, 5.0) * spread
    basis = jnp.clip(jax.random.normal(jax.random.fold_in(key, 12), (ROWS, W), jnp.float32), -5.0, 5.0)
    extra = jnp.exp(jax.random.uniform(jax.random.fold_in(key, 13), (W,), jnp.float32, math.log(2.0), math.log(4.0)))
    dims = (((1,), (1,)), ((), ()))
    schur = lax.dot_general(basis, basis[:W], dims, precision=lax.Precision.HIGHEST, preferred_element_type=jnp.float32) / W
    schur = schur.at[:W].add(jnp.diag(extra))
    whole = lax.dot_general(past, past[:W], dims, precision=lax.Precision.HIGHEST, preferred_element_type=jnp.float32) + schur
    return (whole, past)


def draw_a_cols(key, part):
    return shared_draw(key)[0]


def draw_past_panels(key, part):
    return shared_draw(key)[1]


def setup_inputs(seed: int = 0) -> dict:
    key_of = jax.random.split(jax.random.key(seed), 3)
    a_cols = draw_a_cols(jax.random.fold_in(key_of[2], 71), 0)
    past_panels = draw_past_panels(jax.random.fold_in(key_of[2], 71), 0)
    return {"a_cols": a_cols, "past_panels": past_panels}


def outer_rows(left, right):
    return lax.dot_general(left.astype(jnp.float32), right.astype(jnp.float32), (((1,), (1,)), ((), ())), precision=lax.Precision.HIGHEST, preferred_element_type=jnp.float32)

def reference(a_cols, past_panels):
    result = jnp.zeros((ROWS, W), jnp.float32)
    row_ids = jnp.arange(ROWS, dtype=jnp.int32)[:, None]
    col_ids = jnp.arange(NB, dtype=jnp.int32)[None, :]
    for section in range(STEPS):
        start = section * NB
        summed = outer_rows(past_panels, past_panels[start:start + NB])
        if section > 0:
            summed = summed + outer_rows(result[:, :start], result[start:start + NB, :start])
        update = a_cols[:, start:start + NB] - summed
        diag_factor = jnp.linalg.cholesky(update[start:start + NB])
        solved = jax.scipy.linalg.solve_triangular(diag_factor, update.T, lower=True).T
        new_panel = jnp.where(row_ids >= start + col_ids, solved, jnp.float32(0.0))
        result = result.at[:, start:start + NB].set(new_panel)
    return result
```

```python
import functools

import jax
import jax.numpy as jnp
from jax import lax
from jax.experimental import pallas as pl
from jax.experimental.pallas import tpu as pltpu
from jax.sharding import Mesh
from jax.sharding import PartitionSpec as P

W = 1024
B = 128
NBLK = W // B
PANEL = 16
AXES = ("row", "col_0", "col_1", "depth")
ROW_COL = ("row", "col_0", "col_1")
NT = (((1,), (1,)), ((), ()))
NN = (((1,), (0,)), ((), ()))
f32 = jnp.float32
bf16 = jnp.bfloat16
MESH = pl.DeviceIdType.MESH
VMEM = pl.BlockSpec(memory_space=pltpu.VMEM)


def tile_index(i, j):
    if i < 4:
        return i * (i + 1) // 2 + j
    if j < 4:
        return 10 + (i - 4) * 4 + j if i < 6 else 28 + (i - 6) * 4 + j
    return 18 + (i - 4) * (i - 3) // 2 + (j - 4)


def split(x):
    high = x.astype(bf16)
    return high, (x - high.astype(f32)).astype(bf16)


def dot3(a, b, dims=NT):
    dot = functools.partial(
        lax.dot_general, dimension_numbers=dims, preferred_element_type=f32
    )
    return dot(a[0], b[0]) + (dot(a[0], b[1]) + dot(a[1], b[0]))


def tiles_kernel(own_ref, other_ref, a_ref, out_ref):
    core = lax.axis_index("col_1")
    first = lax.axis_index("depth") == 0
    own = split(own_ref[...])
    square = dot3(own, own)

    def put(place, mat, value):
        out_ref[place] = jnp.where(first, mat, 0.0) - value

    @pl.when(core == 0)
    def _():
        for i in range(4):
            for j in range(i + 1):
                s = square[i * B : i * B + B, j * B : j * B + B]
                put(i * (i + 1) // 2 + j, a_ref[i * B : i * B + B, j * B : j * B + B], s)
        cross = dot3(split(other_ref[0:256, :]), own)
        for i in range(2):
            for j in range(4):
                at = a_ref[j * B : j * B + B, 512 + i * B : 512 + i * B + B].T
                put(10 + i * 4 + j, at, cross[i * B : i * B + B, j * B : j * B + B])

    @pl.when(core == 1)
    def _():
        for i in range(4):
            for j in range(i + 1):
                s = square[i * B : i * B + B, j * B : j * B + B]
                at = a_ref[i * B : i * B + B, 512 + j * B : 512 + j * B + B]
                put(i * (i + 1) // 2 + j, at, s)
        cross = dot3(split(own_ref[256:512, :]), split(other_ref[...]))
        for i in range(2):
            for j in range(4):
                at = a_ref[256 + i * B : 256 + i * B + B, j * B : j * B + B]
                put(10 + i * 4 + j, at, cross[i * B : i * B + B, j * B : j * B + B])


def top_tiles(own, other, a_cols):
    return pl.pallas_call(
        tiles_kernel,
        out_shape=jax.ShapeDtypeStruct((18, B, B), f32),
        in_specs=[VMEM] * 3,
        out_specs=VMEM,
        name="top_tiles",
    )(own, other, a_cols)


def spread_kernel(
    s_ref, t_ref, so_ref, to_ref, ybuf,
    sc_send_s, sc_send_t, sc_recv, y_send, y_recv,
    z_send, z_recv, x_send, x_recv, d_send, d_recv, loc,
):
    x = lax.axis_index("row")
    z = lax.axis_index("col_0")
    c = lax.axis_index("col_1")
    y = lax.axis_index("depth")
    me = x * 8 + z
    left = lax.rem(x + 3, 4)
    right = lax.rem(x + 1, 4)
    far = lax.rem(x + 2, 4)
    root = me == 0
    barrier = pltpu.get_barrier_semaphore()

    def greet(*device):
        pl.semaphore_signal(barrier, inc=1, device_id=device, device_id_type=MESH)

    def z_greet(k, carry):
        greet(x, lax.rem(z + k, 8), c, y)
        return carry

    lax.fori_loop(1, 8, z_greet, 0)
    for k in range(1, 4):
        greet(x, z, c, lax.rem(y + k, 4))
    greet(left, z, c, y)
    greet(right, z, c, y)
    greet(x, z, 1 - c, y)

    @pl.when(jnp.logical_not(root))
    def _():
        greet(0, 0, c, y)
        pl.semaphore_wait(barrier, 13)

    @pl.when(root)
    def _():
        pl.semaphore_wait(barrier, 44)

    def remote(src, dst, send, recv, *device):
        return pltpu.make_async_remote_copy(
            src_ref=src, dst_ref=dst, send_sem=send, recv_sem=recv,
            device_id=device, device_id_type=MESH,
        )

    def scatter_s(q):
        return remote(s_ref.at[q], ybuf.at[y], sc_send_s.at[q], sc_recv.at[0], q // 8, lax.rem(q, 8), c, y)

    def scatter_t(q):
        return remote(t_ref.at[q], to_ref.at[c, q], sc_send_t.at[q], sc_recv.at[1], q // 8, lax.rem(q, 8), c, y)

    own_s = pltpu.make_async_copy(s_ref.at[0], ybuf.at[y], loc.at[0])
    own_t = pltpu.make_async_copy(t_ref.at[0], to_ref.at[c, 0], loc.at[1])

    @pl.when(root)
    def _():
        own_s.start()
        own_t.start()

        def go_s(q, carry):
            scatter_s(q).start()
            return carry

        def go_t(q, carry):
            scatter_t(q).start()
            return carry

        lax.fori_loop(1, 32, go_s, 0)
        lax.fori_loop(1, 32, go_t, 0)
        own_s.wait()

    @pl.when(jnp.logical_not(root))
    def _():
        remote(s_ref.at[0], ybuf.at[y], sc_send_s.at[0], sc_recv.at[0], 0, 0, c, y).wait_recv()

    def y_copy(k):
        return remote(ybuf.at[y], ybuf.at[y], y_send.at[k], y_recv.at[y], x, z, c, lax.rem(y + k, 4))

    for k in range(1, 4):
        y_copy(k).start()

    @pl.when(root)
    def _():
        own_t.wait()

    @pl.when(jnp.logical_not(root))
    def _():
        remote(t_ref.at[0], to_ref.at[c, me], sc_send_t.at[0], sc_recv.at[1], 0, 0, c, y).wait_recv()

    def z_copy(out, n, k):
        return remote(out.at[c, me], out.at[c, me], z_send.at[n, k], z_recv.at[n, z], x, lax.rem(z + k, 8), c, y)

    def z_start(out, n):
        def go(k, carry):
            z_copy(out, n, k).start()
            return carry

        lax.fori_loop(1, 8, go, 0)

    def z_wait(out, n):
        def wait(k, carry):
            source = lax.rem(z + k, 8)
            slot = out.at[c, x * 8 + source]
            remote(slot, slot, z_send.at[n, 0], z_recv.at[n, source], x, source, c, y).wait_recv()
            return carry

        lax.fori_loop(1, 8, wait, 0)

    z_start(to_ref, 1)
    for k in range(1, 4):
        source = lax.rem(y + k, 4)
        slot = ybuf.at[source]
        remote(slot, slot, y_send.at[0], y_recv.at[source], x, z, c, source).wait_recv()
    so_ref[c, me] = (ybuf[0] + ybuf[1]) + (ybuf[2] + ybuf[3])
    z_start(so_ref, 0)

    def group(out, g):
        return out.at[c, pl.ds(g * 8, 8)]

    def half(out, g, h):
        return out.at[c, pl.ds(g * 8 + h * 4, 4)]

    def x_copy(out, n, d):
        return remote(group(out, x), group(out, x), x_send.at[n, d], x_recv.at[n, d], (right, left)[d], z, c, y)

    def relay(out, n, d):
        part = half(out, (left, right)[d], d)
        return remote(part, part, x_send.at[n, 2 + d], x_recv.at[n, 2 + d], (right, left)[d], z, c, y)

    def cross(out, n, k):
        g = (x, left, right, far)[k]
        return remote(group(out, g), group(out, g), d_send.at[n, k], d_recv.at[n, k], x, z, 1 - c, y)

    pair = ((to_ref, 1), (so_ref, 0))
    for out, n in pair:
        z_wait(out, n)
        x_copy(out, n, 0).start()
        x_copy(out, n, 1).start()
        cross(out, n, 0).start()
    for out, n in pair:
        for d in range(2):
            g = (left, right)[d]
            remote(group(out, g), group(out, g), x_send.at[n, d], x_recv.at[n, d], g, z, c, y).wait_recv()
            relay(out, n, d).start()
            cross(out, n, 1 + d).start()
    for out, n in pair:
        for d in range(2):
            part = half(out, far, d)
            remote(part, part, x_send.at[n, 2 + d], x_recv.at[n, 2 + d], (left, right)[d], z, c, y).wait_recv()
        cross(out, n, 3).start()
    for out, n in pair:
        for k in range(4):
            slot = out.at[1 - c, pl.ds((x, left, right, far)[k] * 8, 8)]
            remote(slot, slot, d_send.at[n, k], d_recv.at[n, k], x, z, 1 - c, y).wait_recv()

    @pl.when(root)
    def _():
        def done_s(q, carry):
            scatter_s(q).wait_send()
            scatter_t(q).wait_send()
            return carry

        lax.fori_loop(1, 32, done_s, 0)

    for k in range(1, 4):
        y_copy(k).wait_send()
    for out, n in pair:
        def done_z(k, carry):
            z_copy(out, n, k).wait_send()
            return carry

        lax.fori_loop(1, 8, done_z, 0)
        for d in range(2):
            x_copy(out, n, d).wait_send()
            relay(out, n, d).wait_send()
        for k in range(4):
            cross(out, n, k).wait_send()


def spread(tiles, rows):
    dma = pltpu.SemaphoreType.DMA
    return pl.pallas_call(
        spread_kernel,
        out_shape=(
            jax.ShapeDtypeStruct((2, 32, 72, B), f32),
            jax.ShapeDtypeStruct((2, 32, 16, 512), f32),
        ),
        in_specs=[VMEM] * 2,
        out_specs=(VMEM, VMEM),
        scratch_shapes=[
            pltpu.VMEM((4, 72, B), f32),
            dma((32,)), dma((32,)), dma((2,)), dma((4,)), dma((4,)),
            dma((2, 8)), dma((2, 8)), dma((2, 4)), dma((2, 4)), dma((2, 4)), dma((2, 4)),
            dma((2,)),
        ],
        compiler_params=pltpu.CompilerParams(collective_id=0, has_side_effects=True),
        name="spread",
    )(tiles.reshape(32, 72, B), rows.reshape(32, 16, 512))


def update_kernel(p_ref, t_ref, out_ref):
    mine = split(p_ref[...])
    for n in range(4):
        top = split(t_ref[n * 256 : n * 256 + 256, :])
        out_ref[:, n * 256 : n * 256 + 256] = dot3(mine, top)


def update_part(past, top):
    return pl.pallas_call(
        update_kernel,
        out_shape=jax.ShapeDtypeStruct((512, W), f32),
        in_specs=[VMEM] * 2,
        out_specs=VMEM,
        name="update_part",
    )(past, top)


def row_of(v, m):
    return jnp.broadcast_to(v[m : m + 1, :], v.shape)


def inverse_factor(w, fill):
    lane = lax.broadcasted_iota(jnp.int32, (8, B), 1)
    sub = lax.broadcasted_iota(jnp.int32, (8, B), 0)
    k, kg, n = PANEL, PANEL // 8, B // 8
    w = list(w)
    for t in range(B // k):
        r0, g0 = t * k, t * kg
        cols = [
            [jnp.broadcast_to(w[g][:, r0 + m : r0 + m + 1], (8, B)) for g in range(g0, n)]
            for m in range(k)
        ]
        in_panel = (lane >= r0) & (lane < r0 + k)
        for g in range(g0, n):
            unit = jnp.where(lane == sub + 8 * g, 1.0, 0.0) if g < g0 + kg else jnp.zeros((8, B), f32)
            w[g] = jnp.where(in_panel, unit, w[g])
        piv = [[cols[m][g] for g in range(kg)] for m in range(k)]
        rows = [w[g0 + g] for g in range(kg)]
        final = [None] * k
        for m in range(k):
            gm, sm = divmod(m, 8)
            inv = lax.rsqrt(row_of(piv[m][gm], sm))
            inv2 = inv * inv
            row = row_of(rows[gm], sm)
            final[m] = row * inv
            step = row * inv2
            for g in range(kg):
                new = rows[g] - piv[m][g] * step
                rows[g] = jnp.where(sub == sm, step, new) if g == gm else new
            for m2 in range(m + 1, k):
                f = row_of(piv[m2][gm], sm) * inv2
                for g in range(kg):
                    new = piv[m2][g] - piv[m][g] * f
                    piv[m2][g] = jnp.where(sub == sm, f, new) if g == gm else new
        for g in range(kg):
            acc = final[8 * g]
            for s in range(1, 8):
                acc = jnp.where(sub == s, final[8 * g + s], acc)
            w[g0 + g] = acc
        spread_rows = [row_of(rows[m // 8], m % 8) for m in range(k)]
        for g in range(g0 + kg, n):
            acc = w[g]
            for m in range(k):
                acc = acc - cols[m][g - g0] * spread_rows[m]
            w[g] = acc
        fill(t)
    return [jnp.where(lane <= sub + 8 * g, w[g], 0.0) for g in range(n)]


def factor_kernel(s_ref, lh_ref, ll_ref, dh_ref, dl_ref, a_ref):
    def rows(i, n=1):
        return slice(i * B, (i + n) * B)

    for i in range(NBLK):
        for j in range(i + 1):
            a_ref[rows(i), rows(j)] = s_ref[tile_index(i, j)]

    def low(i, n, j):
        return lh_ref[rows(i, n), rows(j)], ll_ref[rows(i, n), rows(j)]

    def panel(i, n, s, d):
        high, lo = split(dot3(split(a_ref[rows(i, n), rows(s)]), d))
        lh_ref[rows(i, n), rows(s)] = high
        ll_ref[rows(i, n), rows(s)] = lo

    def trail(i, n, j, nj, s):
        a_ref[rows(i, n), rows(j, nj)] -= dot3(low(i, n, s), low(j, nj, s))

    waiting = []
    halves = [None, None]
    for s in range(NBLK):
        def fill(t):
            n = -(-len(waiting) // (8 - t))
            for _ in range(n):
                waiting.pop(0)()

        w = [a_ref[s * B + 8 * g : s * B + 8 * g + 8, rows(s)] for g in range(16)]
        w = inverse_factor(w, fill)
        d32 = jnp.concatenate(w, axis=0)
        d = split(d32)
        halves[s % 2] = d
        at = (s % 2) * B
        dh_ref[s // 2, at : at + B, at : at + B] = d[0]
        dl_ref[s // 2, at : at + B, at : at + B] = d[1]
        if s % 2 == 0:
            dh_ref[s // 2, 0:B, B : 2 * B] = jnp.zeros((B, B), bf16)
            dl_ref[s // 2, 0:B, B : 2 * B] = jnp.zeros((B, B), bf16)
        if s + 1 < NBLK:
            panel(s + 1, 1, s, d)
            trail(s + 1, 1, s + 1, 1, s)
        if s + 2 < NBLK:
            def rest(s=s, d=d):
                panel(s + 2, NBLK - s - 2, s, d)

            waiting.append(rest)
            waiting.append(functools.partial(trail, s + 2, NBLK - s - 2, s + 1, 1, s))
            for j in range(s + 2, NBLK):
                waiting.append(functools.partial(trail, j, NBLK - j, j, 1, s))
        if s % 2 == 1:
            def corner(s=s, first=halves[0], second=halves[1]):
                mid = dot3(low(s, 1, s - 1), first, NN)
                high, lo = split(-dot3(second, split(mid), NN))
                dh_ref[s // 2, B : 2 * B, 0:B] = high
                dl_ref[s // 2, B : 2 * B, 0:B] = lo

            waiting.append(corner)
    for job in waiting:
        job()


def factor_top(tiles):
    return pl.pallas_call(
        factor_kernel,
        out_shape=(
            jax.ShapeDtypeStruct((W, W), bf16),
            jax.ShapeDtypeStruct((W, W), bf16),
            jax.ShapeDtypeStruct((4, 256, 256), bf16),
            jax.ShapeDtypeStruct((4, 256, 256), bf16),
        ),
        in_specs=[VMEM],
        out_specs=(VMEM,) * 4,
        scratch_shapes=[pltpu.VMEM((W, W), f32)],
        cost_estimate=pl.CostEstimate(flops=10**11, bytes_accessed=7 * 2**20, transcendentals=0),
        name="factor_top",
    )(tiles)


def solve_kernel(u0, u1, u2, u3, lh_ref, ll_ref, dh_ref, dl_ref, out_ref, acc, xh, xl):
    depth = lax.axis_index("depth")
    x, z, c = (lax.axis_index(a) for a in ROW_COL)
    base = (x * 16 + z * 2 + c) * 512
    for q, u in enumerate((u0, u1, u2, u3)):
        acc[q * B : q * B + B, :] = u[...]
    for n in range(4):
        cols = slice(n * 256, n * 256 + 256)
        u = acc[:, cols]
        if n:
            done = slice(0, n * 256)
            u = u - dot3((xh[:, done], xl[:, done]), (lh_ref[cols, done], ll_ref[cols, done]))
        out = dot3(split(u), (dh_ref[n], dl_ref[n]))
        xh[:, cols], xl[:, cols] = split(out)
        col = lax.broadcasted_iota(jnp.int32, (B, 256), 1) + n * 256
        for q in range(4):
            place = pl.multiple_of(lax.rem(depth + 4 - q, 4) * B, B)
            row = lax.broadcasted_iota(jnp.int32, (B, 256), 0) + (base + place)
            out_ref[pl.ds(place, B), cols] = jnp.where(row >= col, out[q * B : q * B + B, :], 0.0)


def solve(parts, lower):
    return pl.pallas_call(
        solve_kernel,
        out_shape=jax.ShapeDtypeStruct((512, W), f32),
        in_specs=[VMEM] * 8,
        out_specs=VMEM,
        scratch_shapes=[pltpu.VMEM((512, W), f32), pltpu.VMEM((512, W), bf16), pltpu.VMEM((512, W), bf16)],
        name="solve",
    )(*parts, *lower)


def shift(value, k):
    return lax.ppermute(value, "depth", [(i, (i + k) % 4) for i in range(4)])


def body(a_cols, past):
    depth = lax.axis_index("depth")
    other = lax.ppermute(past, "col_1", [(0, 1), (1, 0)])
    tiles = top_tiles(past, other, a_cols)
    all_tiles, top = spread(tiles, past)
    part = update_part(past, top.reshape(W, 512)).reshape(4, B, W)

    def quarter(array, k):
        return lax.dynamic_index_in_dim(array, (depth + k) % 4, 0, keepdims=False)

    received = [shift(quarter(part, k), k) for k in range(1, 4)]
    summed = quarter(part, 0) + received[0] + received[1] + received[2]
    mine = quarter(a_cols.reshape(4, B, W), 0) - summed
    parts = [mine] + [shift(mine, k) for k in range(1, 4)]
    lower = factor_top(all_tiles.reshape(36, B, B))
    return solve(parts, lower)


def solution(mesh):
    split_mesh = Mesh(
        mesh.devices.reshape(mesh.shape["row"], 8, 2, mesh.shape["depth"]), AXES
    )
    placed = (P(ROW_COL, None), P(ROW_COL, "depth"))
    return jax.shard_map(
        body, mesh=split_mesh, in_specs=placed, out_specs=P(ROW_COL, None), check_vma=False
    )
```

```python
import functools

import jax
import jax.numpy as jnp
from jax import lax
from jax.experimental import pallas as pl
from jax.experimental.pallas import tpu as pltpu
from jax.sharding import Mesh
from jax.sharding import PartitionSpec as P

W = 1024
B = 128
NBLK = W // B
PANEL = 16
AXES = ("row", "col_0", "col_1", "depth")
ROW_COL = ("row", "col_0", "col_1")
NT = (((1,), (1,)), ((), ()))
NN = (((1,), (0,)), ((), ()))
f32 = jnp.float32
bf16 = jnp.bfloat16
MESH = pl.DeviceIdType.MESH
VMEM = pl.BlockSpec(memory_space=pltpu.VMEM)


def tile_index(i, j):
    if i < 4:
        return i * (i + 1) // 2 + j
    if j < 4:
        return 10 + (i - 4) * 4 + j if i < 6 else 28 + (i - 6) * 4 + j
    return 18 + (i - 4) * (i - 3) // 2 + (j - 4)


def split(x):
    high = x.astype(bf16)
    return high, (x - high.astype(f32)).astype(bf16)


def dot3(a, b, dims=NT):
    dot = functools.partial(
        lax.dot_general, dimension_numbers=dims, preferred_element_type=f32
    )
    return dot(a[0], b[0]) + (dot(a[0], b[1]) + dot(a[1], b[0]))


def top_tiles(core, first, past_ref, other_ref, a_ref, tiles_ref):
    own = split(past_ref[...])
    square = dot3(own, own)

    def put(place, mat, value):
        tiles_ref[place * B : place * B + B, :] = jnp.where(first, mat, 0.0) - value

    def part(i, j):
        return slice(i * B, i * B + B), slice(j * B, j * B + B)

    @pl.when(core == 0)
    def _():
        for i in range(4):
            for j in range(i + 1):
                put(i * (i + 1) // 2 + j, a_ref[part(i, j)], square[part(i, j)])
        cross = dot3(split(other_ref[0:256, :]), own)
        for i in range(2):
            for j in range(4):
                put(10 + i * 4 + j, a_ref[part(j, 4 + i)].T, cross[part(i, j)])

    @pl.when(core == 1)
    def _():
        for i in range(4):
            for j in range(i + 1):
                put(i * (i + 1) // 2 + j, a_ref[part(i, 4 + j)], square[part(i, j)])
        cross = dot3(split(past_ref[256:512, :]), split(other_ref[...]))
        for i in range(2):
            for j in range(4):
                put(10 + i * 4 + j, a_ref[part(2 + i, j)], cross[part(i, j)])


def spread_kernel(
    past_ref, a_ref, so_ref, u_ref,
    to_ref, other_ref, tiles_ref, ybuf, th_ref, tl_ref, part_ref, half_ref, full_ref,
    sc_send_s, sc_send_t, sc_recv, y_send, y_recv,
    z_send, z_recv, x_send, x_recv, d_send, d_recv, r_send, r_recv, loc, swap,
):
    x = lax.axis_index("row")
    z = lax.axis_index("col_0")
    c = lax.axis_index("col_1")
    y = lax.axis_index("depth")
    me = x * 8 + z
    left = lax.rem(x + 3, 4)
    right = lax.rem(x + 1, 4)
    far = lax.rem(x + 2, 4)
    down = lax.rem(y + 3, 4)
    up = lax.rem(y + 1, 4)
    across = lax.rem(y + 2, 4)
    root = me == 0
    barrier = pltpu.get_barrier_semaphore()

    def greet(*device):
        pl.semaphore_signal(barrier, inc=1, device_id=device, device_id_type=MESH)

    def z_greet(k, carry):
        greet(x, lax.rem(z + k, 8), c, y)
        return carry

    lax.fori_loop(1, 8, z_greet, 0)
    for k in range(1, 4):
        greet(x, z, c, lax.rem(y + k, 4))
    greet(left, z, c, y)
    greet(right, z, c, y)
    greet(x, z, 1 - c, y)

    @pl.when(jnp.logical_not(root))
    def _():
        greet(0, 0, c, y)
        pl.semaphore_wait(barrier, 13)

    @pl.when(root)
    def _():
        pl.semaphore_wait(barrier, 44)

    def remote(src, dst, send, recv, *device):
        return pltpu.make_async_remote_copy(
            src_ref=src, dst_ref=dst, send_sem=send, recv_sem=recv,
            device_id=device, device_id_type=MESH,
        )

    size = (72, 16)
    full = (so_ref, to_ref)
    pair = (1, 0)

    def pieces(n, core, start, count):
        rows = size[n]
        return full[n].at[pl.ds(pl.multiple_of((core * 32 + start) * rows, 8), count * rows)]

    def source(n, q):
        ref = (tiles_ref, past_ref)[n]
        return ref.at[pl.ds(pl.multiple_of(q * size[n], 8), size[n])]

    def scatter(n, q):
        dst = ybuf.at[y] if n == 0 else pieces(1, c, q, 1)
        send = (sc_send_s, sc_send_t)[n]
        return remote(source(n, q), dst, send.at[q], sc_recv.at[n], q // 8, lax.rem(q, 8), c, y)

    def scatter_all(n):
        def go(q, carry):
            scatter(n, q).start()
            return carry

        lax.fori_loop(1, 32, go, 0)

    def scatter_wait(n):
        dst = ybuf.at[y] if n == 0 else pieces(1, c, me, 1)
        send = (sc_send_s, sc_send_t)[n]
        remote(source(n, 0), dst, send.at[0], sc_recv.at[n], 0, 0, c, y).wait_recv()

    def z_copy(n, k):
        mine = pieces(n, c, me, 1)
        return remote(mine, mine, z_send.at[n, k], z_recv.at[n, z], x, lax.rem(z + k, 8), c, y)

    def z_start(n):
        def go(k, carry):
            z_copy(n, k).start()
            return carry

        lax.fori_loop(1, 8, go, 0)

    def z_wait(n):
        def wait(k, carry):
            peer = lax.rem(z + k, 8)
            slot = pieces(n, c, x * 8 + peer, 1)
            remote(slot, slot, z_send.at[n, 0], z_recv.at[n, peer], x, peer, c, y).wait_recv()
            return carry

        lax.fori_loop(1, 8, wait, 0)

    def group(n, core, g):
        return pieces(n, core, g * 8, 8)

    def half(n, g, h):
        return pieces(n, c, g * 8 + h * 4, 4)

    def x_copy(n, d):
        mine = group(n, c, x)
        return remote(mine, mine, x_send.at[n, d], x_recv.at[n, d], (right, left)[d], z, c, y)

    def x_wait(n, d):
        g = (left, right)[d]
        slot = group(n, c, g)
        remote(slot, slot, x_send.at[n, d], x_recv.at[n, d], g, z, c, y).wait_recv()

    def relay(n, d):
        part = half(n, (left, right)[d], d)
        return remote(part, part, x_send.at[n, 2 + d], x_recv.at[n, 2 + d], (right, left)[d], z, c, y)

    def relay_wait(n, d):
        slot = half(n, far, d)
        remote(slot, slot, x_send.at[n, 2 + d], x_recv.at[n, 2 + d], (left, right)[d], z, c, y).wait_recv()

    order = (x, left, right, far)

    def cross(n, k):
        slot = group(n, c, order[k])
        return remote(slot, slot, d_send.at[n, k], d_recv.at[n, k], x, z, 1 - c, y)

    def cross_wait(n, k):
        slot = group(n, 1 - c, order[k])
        remote(slot, slot, d_send.at[n, k], d_recv.at[n, k], x, z, 1 - c, y).wait_recv()

    trade = remote(past_ref, other_ref, swap.at[0], swap.at[1], x, z, 1 - c, y)
    own_t = pltpu.make_async_copy(source(1, 0), pieces(1, c, 0, 1), loc.at[0])
    own_s = pltpu.make_async_copy(source(0, 0), ybuf.at[y], loc.at[1])

    @pl.when(root)
    def _():
        trade.start()
        own_t.start()
        scatter_all(1)
        own_t.wait()
        z_start(1)
        trade.wait_recv()
        top_tiles(c, y == 0, past_ref, other_ref, a_ref, tiles_ref)
        own_s.start()
        scatter_all(0)
        own_s.wait()

    @pl.when(jnp.logical_not(root))
    def _():
        scatter_wait(1)
        z_start(1)

    z_wait(1)
    for d in range(2):
        x_copy(1, d).start()
    cross(1, 0).start()

    @pl.when(jnp.logical_not(root))
    def _():
        scatter_wait(0)

    def y_copy(k):
        return remote(ybuf.at[y], ybuf.at[y], y_send.at[k], y_recv.at[y], x, z, c, lax.rem(y + k, 4))

    for k in range(1, 4):
        y_copy(k).start()
    for d in range(2):
        x_wait(1, d)
        relay(1, d).start()
        cross(1, 1 + d).start()
    for k in range(1, 4):
        peer = lax.rem(y + k, 4)
        slot = ybuf.at[peer]
        remote(slot, slot, y_send.at[0], y_recv.at[peer], x, z, c, peer).wait_recv()
    so_ref[pl.ds(pl.multiple_of((c * 32 + me) * 72, 8), 72), :] = (ybuf[0] + ybuf[1]) + (ybuf[2] + ybuf[3])
    z_start(0)
    for d in range(2):
        relay_wait(1, d)
    cross(1, 3).start()
    for k in range(4):
        cross_wait(1, k)

    th_ref[...], tl_ref[...] = split(to_ref[...])

    def update(k):
        at = pl.multiple_of(lax.rem(y + k, 4) * B, B)
        mine = split(past_ref[pl.ds(at, B), :])
        for n in range(2):
            cols = slice(n * 512, n * 512 + 512)
            part_ref[k, :, cols] = dot3(mine, (th_ref[cols, :], tl_ref[cols, :]))

    def reduce_first(d):
        rows = pl.ds(d * 64, 64)
        return remote(part_ref.at[2, rows], half_ref.at[d], r_send.at[d], r_recv.at[d], x, z, c, (up, down)[d])

    def reduce_own(d):
        rows = pl.ds(64 - d * 64, 64)
        return remote(
            part_ref.at[1 + 2 * d, rows], full_ref.at[d, rows], r_send.at[2 + d], r_recv.at[2 + d],
            x, z, c, (up, down)[d],
        )

    def reduce_sum(d):
        rows = pl.ds(d * 64, 64)
        return remote(
            part_ref.at[1 + 2 * d, rows], full_ref.at[d, rows], r_send.at[4 + d], r_recv.at[4 + d],
            x, z, c, (up, down)[d],
        )

    update(2)
    for d in range(2):
        reduce_first(d).start()
    for d in range(2):
        update(1 + 2 * d)
        reduce_own(d).start()
    z_wait(0)
    for d in range(2):
        x_copy(0, d).start()
    cross(0, 0).start()
    update(0)
    for d in range(2):
        reduce_first(d).wait_recv()
        rows = slice(d * 64, d * 64 + 64)
        part_ref[1 + 2 * d, rows, :] += half_ref[d]
        reduce_sum(d).start()
    for d in range(2):
        x_wait(0, d)
        relay(0, d).start()
        cross(0, 1 + d).start()
    for d in range(2):
        relay_wait(0, d)
    cross(0, 3).start()
    for k in range(4):
        cross_wait(0, k)
    for d in range(2):
        reduce_own(d).wait_recv()
        reduce_sum(d).wait_recv()
    at = pl.multiple_of(y * B, B)
    u_ref[...] = a_ref[pl.ds(at, B), :] - (part_ref[0] + (full_ref[0] + full_ref[1]))

    @pl.when(root)
    def _():
        trade.wait_send()

        def done(q, carry):
            scatter(0, q).wait_send()
            scatter(1, q).wait_send()
            return carry

        lax.fori_loop(1, 32, done, 0)

    for k in range(1, 4):
        y_copy(k).wait_send()
    for n in pair:
        def done_z(k, carry):
            z_copy(n, k).wait_send()
            return carry

        lax.fori_loop(1, 8, done_z, 0)
        for d in range(2):
            x_copy(n, d).wait_send()
            relay(n, d).wait_send()
        for k in range(4):
            cross(n, k).wait_send()
    for d in range(2):
        reduce_first(d).wait_send()
        reduce_own(d).wait_send()
        reduce_sum(d).wait_send()


def spread(past, a_cols):
    dma = pltpu.SemaphoreType.DMA
    return pl.pallas_call(
        spread_kernel,
        out_shape=(
            jax.ShapeDtypeStruct((36 * B, B), f32),
            jax.ShapeDtypeStruct((B, W), f32),
        ),
        in_specs=[VMEM] * 2,
        out_specs=(VMEM, VMEM),
        scratch_shapes=[
            pltpu.VMEM((W, 512), f32),
            pltpu.VMEM((512, 512), f32),
            pltpu.VMEM((18 * B, B), f32),
            pltpu.VMEM((4, 72, B), f32),
            pltpu.VMEM((W, 512), bf16),
            pltpu.VMEM((W, 512), bf16),
            pltpu.VMEM((4, B, W), f32),
            pltpu.VMEM((2, 64, W), f32),
            pltpu.VMEM((2, B, W), f32),
            dma((32,)), dma((32,)), dma((2,)), dma((4,)), dma((4,)),
            dma((2, 8)), dma((2, 8)), dma((2, 4)), dma((2, 4)), dma((2, 4)), dma((2, 4)),
            dma((6,)), dma((6,)), dma((2,)), dma((2,)),
        ],
        compiler_params=pltpu.CompilerParams(collective_id=0, has_side_effects=True),
        name="spread",
    )(past, a_cols)


def row_of(v, m):
    return jnp.broadcast_to(v[m : m + 1, :], v.shape)


def inverse_factor(w, fill):
    lane = lax.broadcasted_iota(jnp.int32, (8, B), 1)
    sub = lax.broadcasted_iota(jnp.int32, (8, B), 0)
    k, kg, n = PANEL, PANEL // 8, B // 8
    w = list(w)
    for t in range(B // k):
        r0, g0 = t * k, t * kg
        cols = [
            [jnp.broadcast_to(w[g][:, r0 + m : r0 + m + 1], (8, B)) for g in range(g0, n)]
            for m in range(k)
        ]
        in_panel = (lane >= r0) & (lane < r0 + k)
        for g in range(g0, n):
            unit = jnp.where(lane == sub + 8 * g, 1.0, 0.0) if g < g0 + kg else jnp.zeros((8, B), f32)
            w[g] = jnp.where(in_panel, unit, w[g])
        piv = [[cols[m][g] for g in range(kg)] for m in range(k)]
        rows = [w[g0 + g] for g in range(kg)]
        final = [None] * k
        for m in range(k):
            gm, sm = divmod(m, 8)
            inv = lax.rsqrt(row_of(piv[m][gm], sm))
            inv2 = inv * inv
            row = row_of(rows[gm], sm)
            final[m] = row * inv
            step = row * inv2
            for g in range(kg):
                new = rows[g] - piv[m][g] * step
                rows[g] = jnp.where(sub == sm, step, new) if g == gm else new
            for m2 in range(m + 1, k):
                f = row_of(piv[m2][gm], sm) * inv2
                for g in range(kg):
                    new = piv[m2][g] - piv[m][g] * f
                    piv[m2][g] = jnp.where(sub == sm, f, new) if g == gm else new
        for g in range(kg):
            acc = final[8 * g]
            for s in range(1, 8):
                acc = jnp.where(sub == s, final[8 * g + s], acc)
            w[g0 + g] = acc
        spread_rows = [row_of(rows[m // 8], m % 8) for m in range(k)]
        for g in range(g0 + kg, n):
            acc = w[g]
            for m in range(k):
                acc = acc - cols[m][g - g0] * spread_rows[m]
            w[g] = acc
        fill(t)
    return [jnp.where(lane <= sub + 8 * g, w[g], 0.0) for g in range(n)]


def factor_kernel(s_ref, lh_ref, ll_ref, dh_ref, dl_ref, a_ref):
    def rows(i, n=1):
        return slice(i * B, (i + n) * B)

    for i in range(NBLK):
        for j in range(i + 1):
            a_ref[rows(i), rows(j)] = s_ref[tile_index(i, j)]

    def low(i, n, j):
        return lh_ref[rows(i, n), rows(j)], ll_ref[rows(i, n), rows(j)]

    def panel(i, n, s, d):
        high, lo = split(dot3(split(a_ref[rows(i, n), rows(s)]), d))
        lh_ref[rows(i, n), rows(s)] = high
        ll_ref[rows(i, n), rows(s)] = lo

    def trail(i, n, j, nj, s):
        a_ref[rows(i, n), rows(j, nj)] -= dot3(low(i, n, s), low(j, nj, s))

    waiting = []
    halves = [None, None]
    for s in range(NBLK):
        def fill(t):
            n = -(-len(waiting) // (8 - t))
            for _ in range(n):
                waiting.pop(0)()

        w = [a_ref[s * B + 8 * g : s * B + 8 * g + 8, rows(s)] for g in range(16)]
        w = inverse_factor(w, fill)
        d32 = jnp.concatenate(w, axis=0)
        d = split(d32)
        halves[s % 2] = d
        at = (s % 2) * B
        dh_ref[s // 2, at : at + B, at : at + B] = d[0]
        dl_ref[s // 2, at : at + B, at : at + B] = d[1]
        if s % 2 == 0:
            dh_ref[s // 2, 0:B, B : 2 * B] = jnp.zeros((B, B), bf16)
            dl_ref[s // 2, 0:B, B : 2 * B] = jnp.zeros((B, B), bf16)
        if s + 1 < NBLK:
            panel(s + 1, 1, s, d)
            trail(s + 1, 1, s + 1, 1, s)
        if s + 2 < NBLK:
            def rest(s=s, d=d):
                panel(s + 2, NBLK - s - 2, s, d)

            waiting.append(rest)
            waiting.append(functools.partial(trail, s + 2, NBLK - s - 2, s + 1, 1, s))
            for j in range(s + 2, NBLK):
                waiting.append(functools.partial(trail, j, NBLK - j, j, 1, s))
        if s % 2 == 1:
            def corner(s=s, first=halves[0], second=halves[1]):
                mid = dot3(low(s, 1, s - 1), first, NN)
                high, lo = split(-dot3(second, split(mid), NN))
                dh_ref[s // 2, B : 2 * B, 0:B] = high
                dl_ref[s // 2, B : 2 * B, 0:B] = lo

            waiting.append(corner)
    for job in waiting:
        job()


def factor_top(tiles):
    return pl.pallas_call(
        factor_kernel,
        out_shape=(
            jax.ShapeDtypeStruct((W, W), bf16),
            jax.ShapeDtypeStruct((W, W), bf16),
            jax.ShapeDtypeStruct((4, 256, 256), bf16),
            jax.ShapeDtypeStruct((4, 256, 256), bf16),
        ),
        in_specs=[VMEM],
        out_specs=(VMEM,) * 4,
        scratch_shapes=[pltpu.VMEM((W, W), f32)],
        cost_estimate=pl.CostEstimate(flops=10**11, bytes_accessed=7 * 2**20, transcendentals=0),
        name="factor_top",
    )(tiles)


def solve_kernel(u0, u1, u2, u3, lh_ref, ll_ref, dh_ref, dl_ref, out_ref, acc, xh, xl):
    depth = lax.axis_index("depth")
    x, z, c = (lax.axis_index(a) for a in ROW_COL)
    base = (x * 16 + z * 2 + c) * 512
    for q, u in enumerate((u0, u1, u2, u3)):
        acc[q * B : q * B + B, :] = u[...]
    for n in range(4):
        cols = slice(n * 256, n * 256 + 256)
        u = acc[:, cols]
        if n:
            done = slice(0, n * 256)
            u = u - dot3((xh[:, done], xl[:, done]), (lh_ref[cols, done], ll_ref[cols, done]))
        out = dot3(split(u), (dh_ref[n], dl_ref[n]))
        xh[:, cols], xl[:, cols] = split(out)
        col = lax.broadcasted_iota(jnp.int32, (B, 256), 1) + n * 256
        for q in range(4):
            place = pl.multiple_of(lax.rem(depth + 4 - q, 4) * B, B)
            row = lax.broadcasted_iota(jnp.int32, (B, 256), 0) + (base + place)
            out_ref[pl.ds(place, B), cols] = jnp.where(row >= col, out[q * B : q * B + B, :], 0.0)


def solve(parts, lower):
    return pl.pallas_call(
        solve_kernel,
        out_shape=jax.ShapeDtypeStruct((512, W), f32),
        in_specs=[VMEM] * 8,
        out_specs=VMEM,
        scratch_shapes=[pltpu.VMEM((512, W), f32), pltpu.VMEM((512, W), bf16), pltpu.VMEM((512, W), bf16)],
        name="solve",
    )(*parts, *lower)


def shift(value, k):
    return lax.ppermute(value, "depth", [(i, (i + k) % 4) for i in range(4)])


def body(a_cols, past):
    tiles, mine = spread(past, a_cols)
    parts = [mine] + [shift(mine, k) for k in range(1, 4)]
    lower = factor_top(tiles.reshape(36, B, B))
    return solve(parts, lower)


def solution(mesh):
    split_mesh = Mesh(
        mesh.devices.reshape(mesh.shape["row"], 8, 2, mesh.shape["depth"]), AXES
    )
    placed = (P(ROW_COL, None), P(ROW_COL, "depth"))
    return jax.shard_map(
        body, mesh=split_mesh, in_specs=placed, out_specs=P(ROW_COL, None), check_vma=False
    )
```

```python
import functools

import jax
import jax.numpy as jnp
from jax import lax
from jax.experimental import pallas as pl
from jax.experimental.pallas import tpu as pltpu
from jax.sharding import Mesh
from jax.sharding import PartitionSpec as P

W = 1024
B = 128
NBLK = W // B
PANEL = 16
AXES = ("row", "col_0", "col_1", "depth")
ROW_COL = ("row", "col_0", "col_1")
NT = (((1,), (1,)), ((), ()))
NN = (((1,), (0,)), ((), ()))
f32 = jnp.float32
bf16 = jnp.bfloat16
MESH = pl.DeviceIdType.MESH
VMEM = pl.BlockSpec(memory_space=pltpu.VMEM)


def tile_index(i, j):
    if i < 4:
        return i * (i + 1) // 2 + j
    if j < 4:
        return 10 + (i - 4) * 4 + j if i < 6 else 28 + (i - 6) * 4 + j
    return 18 + (i - 4) * (i - 3) // 2 + (j - 4)


def split(x):
    high = x.astype(bf16)
    return high, (x - high.astype(f32)).astype(bf16)


def dot3(a, b, dims=NT):
    dot = functools.partial(
        lax.dot_general, dimension_numbers=dims, preferred_element_type=f32
    )
    return dot(a[0], b[0]) + (dot(a[0], b[1]) + dot(a[1], b[0]))


def top_tiles(core, first, past_ref, other_ref, a_ref, tiles_ref):
    own = split(past_ref[...])
    square = dot3(own, own)

    def put(place, mat, value):
        tiles_ref[place * B : place * B + B, :] = jnp.where(first, mat, 0.0) - value

    def part(i, j):
        return slice(i * B, i * B + B), slice(j * B, j * B + B)

    @pl.when(core == 0)
    def _():
        for i in range(4):
            for j in range(i + 1):
                put(i * (i + 1) // 2 + j, a_ref[part(i, j)], square[part(i, j)])
        cross = dot3(split(other_ref[0:256, :]), own)
        for i in range(2):
            for j in range(4):
                put(10 + i * 4 + j, a_ref[part(j, 4 + i)].T, cross[part(i, j)])

    @pl.when(core == 1)
    def _():
        for i in range(4):
            for j in range(i + 1):
                put(i * (i + 1) // 2 + j, a_ref[part(i, 4 + j)], square[part(i, j)])
        cross = dot3(split(past_ref[256:512, :]), split(other_ref[...]))
        for i in range(2):
            for j in range(4):
                put(10 + i * 4 + j, a_ref[part(2 + i, j)], cross[part(i, j)])


def whole_kernel(
    past_ref, a_ref, out_ref,
    so_ref, u_ref, top_ref, lh_ref, ll_ref, dh_ref, dl_ref, xh_ref, xl_ref, g_send, g_recv,
    to_ref, other_ref, tiles_ref, ybuf, th_ref, tl_ref, part_ref, half_ref, full_ref,
    sc_send_s, sc_send_t, sc_recv, y_send, y_recv,
    z_send, z_recv, x_send, x_recv, d_send, d_recv, r_send, r_recv, loc, swap,
):
    x = lax.axis_index("row")
    z = lax.axis_index("col_0")
    c = lax.axis_index("col_1")
    y = lax.axis_index("depth")
    me = x * 8 + z
    left = lax.rem(x + 3, 4)
    right = lax.rem(x + 1, 4)
    far = lax.rem(x + 2, 4)
    down = lax.rem(y + 3, 4)
    up = lax.rem(y + 1, 4)
    across = lax.rem(y + 2, 4)
    root = me == 0
    barrier = pltpu.get_barrier_semaphore()

    def greet(*device):
        pl.semaphore_signal(barrier, inc=1, device_id=device, device_id_type=MESH)

    def z_greet(k, carry):
        greet(x, lax.rem(z + k, 8), c, y)
        return carry

    lax.fori_loop(1, 8, z_greet, 0)
    for k in range(1, 4):
        greet(x, z, c, lax.rem(y + k, 4))
    greet(left, z, c, y)
    greet(right, z, c, y)
    greet(x, z, 1 - c, y)

    @pl.when(jnp.logical_not(root))
    def _():
        greet(0, 0, c, y)
        pl.semaphore_wait(barrier, 13)

    @pl.when(root)
    def _():
        pl.semaphore_wait(barrier, 44)

    def remote(src, dst, send, recv, *device):
        return pltpu.make_async_remote_copy(
            src_ref=src, dst_ref=dst, send_sem=send, recv_sem=recv,
            device_id=device, device_id_type=MESH,
        )

    size = (72, 16)
    full = (so_ref, to_ref)
    pair = (1, 0)

    def pieces(n, core, start, count):
        rows = size[n]
        return full[n].at[pl.ds(pl.multiple_of((core * 32 + start) * rows, 8), count * rows)]

    def source(n, q):
        ref = (tiles_ref, past_ref)[n]
        return ref.at[pl.ds(pl.multiple_of(q * size[n], 8), size[n])]

    def scatter(n, q):
        dst = ybuf.at[y] if n == 0 else pieces(1, c, q, 1)
        send = (sc_send_s, sc_send_t)[n]
        return remote(source(n, q), dst, send.at[q], sc_recv.at[n], q // 8, lax.rem(q, 8), c, y)

    def scatter_all(n):
        def go(q, carry):
            scatter(n, q).start()
            return carry

        lax.fori_loop(1, 32, go, 0)

    def scatter_wait(n):
        dst = ybuf.at[y] if n == 0 else pieces(1, c, me, 1)
        send = (sc_send_s, sc_send_t)[n]
        remote(source(n, 0), dst, send.at[0], sc_recv.at[n], 0, 0, c, y).wait_recv()

    def z_copy(n, k):
        mine = pieces(n, c, me, 1)
        return remote(mine, mine, z_send.at[n, k], z_recv.at[n, z], x, lax.rem(z + k, 8), c, y)

    def z_start(n):
        def go(k, carry):
            z_copy(n, k).start()
            return carry

        lax.fori_loop(1, 8, go, 0)

    def z_wait(n):
        def wait(k, carry):
            peer = lax.rem(z + k, 8)
            slot = pieces(n, c, x * 8 + peer, 1)
            remote(slot, slot, z_send.at[n, 0], z_recv.at[n, peer], x, peer, c, y).wait_recv()
            return carry

        lax.fori_loop(1, 8, wait, 0)

    def group(n, core, g):
        return pieces(n, core, g * 8, 8)

    def half(n, g, h):
        return pieces(n, c, g * 8 + h * 4, 4)

    def x_copy(n, d):
        mine = group(n, c, x)
        return remote(mine, mine, x_send.at[n, d], x_recv.at[n, d], (right, left)[d], z, c, y)

    def x_wait(n, d):
        g = (left, right)[d]
        slot = group(n, c, g)
        remote(slot, slot, x_send.at[n, d], x_recv.at[n, d], g, z, c, y).wait_recv()

    def relay(n, d):
        part = half(n, (left, right)[d], d)
        return remote(part, part, x_send.at[n, 2 + d], x_recv.at[n, 2 + d], (right, left)[d], z, c, y)

    def relay_wait(n, d):
        slot = half(n, far, d)
        remote(slot, slot, x_send.at[n, 2 + d], x_recv.at[n, 2 + d], (left, right)[d], z, c, y).wait_recv()

    order = (x, left, right, far)

    def cross(n, k):
        slot = group(n, c, order[k])
        return remote(slot, slot, d_send.at[n, k], d_recv.at[n, k], x, z, 1 - c, y)

    def cross_wait(n, k):
        slot = group(n, 1 - c, order[k])
        remote(slot, slot, d_send.at[n, k], d_recv.at[n, k], x, z, 1 - c, y).wait_recv()

    trade = remote(past_ref, other_ref, swap.at[0], swap.at[1], x, z, 1 - c, y)
    own_t = pltpu.make_async_copy(source(1, 0), pieces(1, c, 0, 1), loc.at[0])
    own_s = pltpu.make_async_copy(source(0, 0), ybuf.at[y], loc.at[1])

    @pl.when(root)
    def _():
        trade.start()
        own_t.start()
        scatter_all(1)
        own_t.wait()
        z_start(1)
        trade.wait_recv()
        top_tiles(c, y == 0, past_ref, other_ref, a_ref, tiles_ref)
        own_s.start()
        scatter_all(0)
        own_s.wait()

    @pl.when(jnp.logical_not(root))
    def _():
        scatter_wait(1)
        z_start(1)

    z_wait(1)
    for d in range(2):
        x_copy(1, d).start()
    cross(1, 0).start()

    @pl.when(jnp.logical_not(root))
    def _():
        scatter_wait(0)

    def y_copy(k):
        return remote(ybuf.at[y], ybuf.at[y], y_send.at[k], y_recv.at[y], x, z, c, lax.rem(y + k, 4))

    for k in range(1, 4):
        y_copy(k).start()
    for d in range(2):
        x_wait(1, d)
        relay(1, d).start()
        cross(1, 1 + d).start()
    for k in range(1, 4):
        peer = lax.rem(y + k, 4)
        slot = ybuf.at[peer]
        remote(slot, slot, y_send.at[0], y_recv.at[peer], x, z, c, peer).wait_recv()
    so_ref[pl.ds(pl.multiple_of((c * 32 + me) * 72, 8), 72), :] = (ybuf[0] + ybuf[1]) + (ybuf[2] + ybuf[3])
    z_start(0)
    for d in range(2):
        relay_wait(1, d)
    cross(1, 3).start()
    for k in range(4):
        cross_wait(1, k)

    th_ref[...], tl_ref[...] = split(to_ref[...])

    def update(k):
        at = pl.multiple_of(lax.rem(y + k, 4) * B, B)
        mine = split(past_ref[pl.ds(at, B), :])
        for n in range(2):
            cols = slice(n * 512, n * 512 + 512)
            part_ref[k, :, cols] = dot3(mine, (th_ref[cols, :], tl_ref[cols, :]))

    def reduce_first(d):
        rows = pl.ds(d * 64, 64)
        return remote(part_ref.at[2, rows], half_ref.at[d], r_send.at[d], r_recv.at[d], x, z, c, (up, down)[d])

    def reduce_own(d):
        rows = pl.ds(64 - d * 64, 64)
        return remote(
            part_ref.at[1 + 2 * d, rows], full_ref.at[d, rows], r_send.at[2 + d], r_recv.at[2 + d],
            x, z, c, (up, down)[d],
        )

    def reduce_sum(d):
        rows = pl.ds(d * 64, 64)
        return remote(
            part_ref.at[1 + 2 * d, rows], full_ref.at[d, rows], r_send.at[4 + d], r_recv.at[4 + d],
            x, z, c, (up, down)[d],
        )

    update(2)
    for d in range(2):
        reduce_first(d).start()
    for d in range(2):
        update(1 + 2 * d)
        reduce_own(d).start()
    z_wait(0)
    for d in range(2):
        x_copy(0, d).start()
    cross(0, 0).start()
    update(0)
    for d in range(2):
        reduce_first(d).wait_recv()
        rows = slice(d * 64, d * 64 + 64)
        part_ref[1 + 2 * d, rows, :] += half_ref[d]
        reduce_sum(d).start()
    for d in range(2):
        x_wait(0, d)
        relay(0, d).start()
        cross(0, 1 + d).start()
    for d in range(2):
        relay_wait(0, d)
    cross(0, 3).start()
    for k in range(4):
        cross_wait(0, k)
    for d in range(2):
        reduce_own(d).wait_recv()
        reduce_sum(d).wait_recv()
    at = pl.multiple_of(y * B, B)
    u_ref[0:B, :] = a_ref[pl.ds(at, B), :] - (part_ref[0] + (full_ref[0] + full_ref[1]))

    def gather(d):
        to = pl.ds((1 + 2 * d) * B, B)
        return remote(u_ref.at[pl.ds(0, B)], u_ref.at[to], g_send.at[d], g_recv.at[d], x, z, c, (up, down)[d])

    def gather_on(d):
        mine = pl.ds((1 + 2 * d) * B + d * 64, 64)
        to = pl.ds(2 * B + d * 64, 64)
        return remote(u_ref.at[mine], u_ref.at[to], g_send.at[2 + d], g_recv.at[2 + d], x, z, c, (up, down)[d])

    for d in range(2):
        gather(d).start()

    def pass_on():
        for d in range(2):
            gather(d).wait_recv()
            gather_on(d).start()

    factor_top(so_ref, lh_ref, ll_ref, dh_ref, dl_ref, top_ref, {4: pass_on})
    for d in range(2):
        gather_on(d).wait_recv()
    solve(y, (x * 16 + z * 2 + c) * 512, u_ref, lh_ref, ll_ref, dh_ref, dl_ref, out_ref, xh_ref, xl_ref)

    @pl.when(root)
    def _():
        trade.wait_send()

        def done(q, carry):
            scatter(0, q).wait_send()
            scatter(1, q).wait_send()
            return carry

        lax.fori_loop(1, 32, done, 0)

    for k in range(1, 4):
        y_copy(k).wait_send()
    for n in pair:
        def done_z(k, carry):
            z_copy(n, k).wait_send()
            return carry

        lax.fori_loop(1, 8, done_z, 0)
        for d in range(2):
            x_copy(n, d).wait_send()
            relay(n, d).wait_send()
        for k in range(4):
            cross(n, k).wait_send()
    for d in range(2):
        reduce_first(d).wait_send()
        reduce_own(d).wait_send()
        reduce_sum(d).wait_send()
        gather(d).wait_send()
        gather_on(d).wait_send()


def whole(past, a_cols):
    dma = pltpu.SemaphoreType.DMA
    return pl.pallas_call(
        whole_kernel,
        out_shape=jax.ShapeDtypeStruct((512, W), f32),
        in_specs=[VMEM] * 2,
        out_specs=VMEM,
        scratch_shapes=[
            pltpu.VMEM((36 * B, B), f32),
            pltpu.VMEM((4 * B, W), f32),
            pltpu.VMEM((W, W), f32),
            pltpu.VMEM((W, W), bf16),
            pltpu.VMEM((W, W), bf16),
            pltpu.VMEM((4, 256, 256), bf16),
            pltpu.VMEM((4, 256, 256), bf16),
            pltpu.VMEM((4 * B, W), bf16),
            pltpu.VMEM((4 * B, W), bf16),
            dma((4,)), dma((4,)),
            pltpu.VMEM((W, 512), f32),
            pltpu.VMEM((512, 512), f32),
            pltpu.VMEM((18 * B, B), f32),
            pltpu.VMEM((4, 72, B), f32),
            pltpu.VMEM((W, 512), bf16),
            pltpu.VMEM((W, 512), bf16),
            pltpu.VMEM((4, B, W), f32),
            pltpu.VMEM((2, 64, W), f32),
            pltpu.VMEM((2, B, W), f32),
            dma((32,)), dma((32,)), dma((2,)), dma((4,)), dma((4,)),
            dma((2, 8)), dma((2, 8)), dma((2, 4)), dma((2, 4)), dma((2, 4)), dma((2, 4)),
            dma((6,)), dma((6,)), dma((2,)), dma((2,)),
        ],
        compiler_params=pltpu.CompilerParams(collective_id=0, has_side_effects=True),
        name="whole",
    )(past, a_cols)


def inverse_factor(w, fill):
    lane = lax.broadcasted_iota(jnp.int32, (B, B), 1)
    sub = lax.broadcasted_iota(jnp.int32, (B, B), 0)
    k = PANEL
    at = sub[:k]
    done = []
    for t in range(B // k):
        r0 = t * k
        left = B - r0
        cols = [jnp.broadcast_to(w[:, r0 + m : r0 + m + 1], (left, B)) for m in range(k)]
        lanes, subs = lane[:left], sub[:left]
        unit = jnp.where((lanes == subs + r0) & (subs < k), 1.0, 0.0)
        w = jnp.where((lanes >= r0) & (lanes < r0 + k), unit, w)
        rows = w[:k]
        piv = jnp.stack([col[:k] for col in cols])
        final = jnp.zeros((k, B), f32)
        for m in range(k):
            mine, rest = piv[0], piv[1:]
            inv = lax.rsqrt(jnp.broadcast_to(mine[m : m + 1], (k, B)))
            inv2 = inv * inv
            row = jnp.broadcast_to(rows[m : m + 1], (k, B))
            here = at == m
            final = jnp.where(here, row * inv, final)
            step = row * inv2
            rows = jnp.where(here, step, rows - mine * step)
            if m + 1 < k:
                f = jnp.broadcast_to(rest[:, m : m + 1], (k - 1 - m, k, B)) * inv2[None]
                piv = jnp.where(here[None], f, rest - mine[None] * f)
        done.append(jnp.where(lane[:k] <= at + r0, final, 0.0))
        if left > k:
            w = w[k:]
            for m in range(k):
                w = w - cols[m][k:] * jnp.broadcast_to(rows[m : m + 1], (left - k, B))
        fill(t)
    return jnp.concatenate(done, axis=0)


def factor_top(s_ref, lh_ref, ll_ref, dh_ref, dl_ref, a_ref, events):
    def rows(i, n=1):
        return slice(i * B, (i + n) * B)

    for i in range(NBLK):
        for j in range(i + 1):
            n = tile_index(i, j)
            a_ref[rows(i), rows(j)] = s_ref[rows(n), :]

    def low(i, n, j):
        return lh_ref[rows(i, n), rows(j)], ll_ref[rows(i, n), rows(j)]

    def panel(i, n, s, d):
        high, lo = split(dot3(split(a_ref[rows(i, n), rows(s)]), d))
        lh_ref[rows(i, n), rows(s)] = high
        ll_ref[rows(i, n), rows(s)] = lo

    def trail(i, n, j, nj, s):
        a_ref[rows(i, n), rows(j, nj)] -= dot3(low(i, n, s), low(j, nj, s))

    waiting = []
    halves = [None, None]
    for s in range(NBLK):
        def fill(t):
            n = -(-len(waiting) // (B // PANEL - t))
            for _ in range(n):
                waiting.pop(0)()

        if s in events:
            waiting.append(events[s])
        d = split(inverse_factor(a_ref[rows(s), rows(s)], fill))
        halves[s % 2] = d
        at = (s % 2) * B
        dh_ref[s // 2, at : at + B, at : at + B] = d[0]
        dl_ref[s // 2, at : at + B, at : at + B] = d[1]
        if s % 2 == 0:
            dh_ref[s // 2, 0:B, B : 2 * B] = jnp.zeros((B, B), bf16)
            dl_ref[s // 2, 0:B, B : 2 * B] = jnp.zeros((B, B), bf16)
        if s + 1 < NBLK:
            panel(s + 1, 1, s, d)
            trail(s + 1, 1, s + 1, 1, s)
        if s + 2 < NBLK:
            def rest(s=s, d=d):
                panel(s + 2, NBLK - s - 2, s, d)

            waiting.append(rest)
            waiting.append(functools.partial(trail, s + 2, NBLK - s - 2, s + 1, 1, s))
            for j in range(s + 2, NBLK):
                waiting.append(functools.partial(trail, j, NBLK - j, j, 1, s))
        if s % 2 == 1:
            def corner(s=s, first=halves[0], second=halves[1]):
                mid = dot3(low(s, 1, s - 1), first, NN)
                high, lo = split(-dot3(second, split(mid), NN))
                dh_ref[s // 2, B : 2 * B, 0:B] = high
                dl_ref[s // 2, B : 2 * B, 0:B] = lo

            waiting.append(corner)
    for job in waiting:
        job()


def solve(depth, base, u_ref, lh_ref, ll_ref, dh_ref, dl_ref, out_ref, xh, xl):
    for n in range(4):
        cols = slice(n * 256, n * 256 + 256)
        u = u_ref[:, cols]
        if n:
            done = slice(0, n * 256)
            u = u - dot3((xh[:, done], xl[:, done]), (lh_ref[cols, done], ll_ref[cols, done]))
        out = dot3(split(u), (dh_ref[n], dl_ref[n]))
        xh[:, cols], xl[:, cols] = split(out)
        col = lax.broadcasted_iota(jnp.int32, (B, 256), 1) + n * 256
        for q in range(4):
            place = pl.multiple_of(lax.rem(depth + 4 - q, 4) * B, B)
            row = lax.broadcasted_iota(jnp.int32, (B, 256), 0) + (base + place)
            out_ref[pl.ds(place, B), cols] = jnp.where(row >= col, out[q * B : q * B + B, :], 0.0)


def body(a_cols, past):
    return whole(past, a_cols)


def solution(mesh):
    split_mesh = Mesh(
        mesh.devices.reshape(mesh.shape["row"], 8, 2, mesh.shape["depth"]), AXES
    )
    placed = (P(ROW_COL, None), P(ROW_COL, "depth"))
    return jax.shard_map(
        body, mesh=split_mesh, in_specs=placed, out_specs=P(ROW_COL, None), check_vma=False
    )
```

```python
import functools

import jax
import jax.numpy as jnp
from jax import lax
from jax.experimental import pallas as pl
from jax.experimental.pallas import tpu as pltpu
from jax.sharding import Mesh
from jax.sharding import PartitionSpec as P

W = 1024
B = 128
NBLK = W // B
PANEL = 16
AXES = ("row", "col_0", "col_1", "depth")
ROW_COL = ("row", "col_0", "col_1")
NT = (((1,), (1,)), ((), ()))
NN = (((1,), (0,)), ((), ()))
f32 = jnp.float32
bf16 = jnp.bfloat16
MESH = pl.DeviceIdType.MESH
VMEM = pl.BlockSpec(memory_space=pltpu.VMEM)


TILES = (
    (((0, 0), (1, 0), (2, 0), (3, 0)), ((4, 0), (5, 0), (6, 0), (7, 0))),
    (
        ((1, 1), (2, 1), (3, 1), (2, 2), (3, 2), (3, 3)),
        ((4, 1), (5, 1), (6, 1), (7, 1), (4, 2), (5, 2)),
    ),
    (
        ((6, 2), (7, 2), (4, 3), (5, 3), (6, 3), (7, 3), (4, 4), (5, 4)),
        ((6, 4), (7, 4), (5, 5), (6, 5), (7, 5), (6, 6), (7, 6), (7, 7)),
    ),
)
ROWS = (8, 8, 16, 24, 32)
BASE = (0, 256, 0, 1024, 2560)
STRIDE = (512, 512, 512, 768, 1024)
SOURCE = (0, 256, 0, 512, 1280)
SLOT = (0, 0, 0, 16, 40)


def split(x):
    high = x.astype(bf16)
    return high, (x - high.astype(f32)).astype(bf16)


def dot3(a, b, dims=NT):
    dot = functools.partial(
        lax.dot_general, dimension_numbers=dims, preferred_element_type=f32
    )
    return dot(a[0], b[0]) + (dot(a[0], b[1]) + dot(a[1], b[0]))


def top_tiles(part, core, first, th_ref, tl_ref, a_ref, other_a_ref, tiles_ref):
    out = SOURCE[2 + part]

    def blocks(i, n=1):
        return slice(i * B, (i + n) * B)

    def value(i, j):
        if core == 1:
            return a_ref[blocks(i - 4), blocks(j)]
        if i < 4:
            return a_ref[blocks(i), blocks(j)]
        if j < 4:
            return a_ref[blocks(j), blocks(i)].T
        return other_a_ref[blocks(i - 4), blocks(j - 4)]

    todo = list(TILES[part][core])
    while todo:
        i, j = todo[0]
        n = 1
        while n < len(todo) and todo[n] == (i + n, j):
            n += 1
        todo = todo[n:]
        product = dot3(
            (th_ref[blocks(i, n), :], tl_ref[blocks(i, n), :]),
            (th_ref[blocks(j), :], tl_ref[blocks(j), :]),
        )
        for k in range(n):
            tiles_ref[out : out + B, :] = jnp.where(first, value(i + k, j), 0.0) - product[blocks(k)]
            out += B


def whole_kernel(
    past_ref, a_ref, out_ref,
    so_ref, u_ref, top_ref, lh_ref, ll_ref, dh_ref, dl_ref, xh_ref, xl_ref,
    to_ref, other_ref, other_a_ref, tiles_ref, ybuf, th_ref, tl_ref, part_ref, half_ref, full_ref,
    sc_send, sc_recv, y_send, y_recv, z_send, z_recv, x_send, x_recv, d_send, d_recv,
    r_send, r_recv, g_send, g_recv, loc, swap,
):
    x = lax.axis_index("row")
    z = lax.axis_index("col_0")
    c = lax.axis_index("col_1")
    y = lax.axis_index("depth")
    me = x * 8 + z
    left = lax.rem(x + 3, 4)
    right = lax.rem(x + 1, 4)
    far = lax.rem(x + 2, 4)
    down = lax.rem(y + 3, 4)
    up = lax.rem(y + 1, 4)
    root = me == 0
    barrier = pltpu.get_barrier_semaphore()

    def greet(*device):
        pl.semaphore_signal(barrier, inc=1, device_id=device, device_id_type=MESH)

    def z_greet(k, carry):
        greet(x, lax.rem(z + k, 8), c, y)
        return carry

    lax.fori_loop(1, 8, z_greet, 0)
    for k in range(1, 4):
        greet(x, z, c, lax.rem(y + k, 4))
    greet(left, z, c, y)
    greet(right, z, c, y)
    greet(x, z, 1 - c, y)

    @pl.when(jnp.logical_not(root))
    def _():
        greet(0, 0, c, y)
        pl.semaphore_wait(barrier, 13)

    @pl.when(root)
    def _():
        pl.semaphore_wait(barrier, 44)

    def remote(src, dst, send, recv, *device):
        return pltpu.make_async_remote_copy(
            src_ref=src, dst_ref=dst, send_sem=send, recv_sem=recv,
            device_id=device, device_id_type=MESH,
        )


    def pieces(n, core, start, count):
        at = pl.multiple_of(BASE[n] + core * STRIDE[n] + start * ROWS[n], 8)
        return (to_ref if n < 2 else so_ref).at[pl.ds(at, count * ROWS[n])]

    def slot(n, layer):
        return ybuf.at[layer, pl.ds(SLOT[n], ROWS[n])]

    def source(n, q):
        at = pl.multiple_of(SOURCE[n] + q * ROWS[n], 8)
        return (past_ref if n < 2 else tiles_ref).at[pl.ds(at, ROWS[n])]

    def scatter(n, q):
        dst = pieces(n, c, q, 1) if n < 2 else slot(n, y)
        return remote(source(n, q), dst, sc_send.at[n, q], sc_recv.at[n], q // 8, lax.rem(q, 8), c, y)

    def own(n):
        dst = pieces(n, c, 0, 1) if n < 2 else slot(n, y)
        return pltpu.make_async_copy(source(n, 0), dst, loc.at[n])

    def scatter_all(n):
        own(n).start()

        def go(q, carry):
            scatter(n, q).start()
            return carry

        lax.fori_loop(1, 32, go, 0)
        own(n).wait()

    def scatter_wait(n):
        @pl.when(jnp.logical_not(root))
        def _():
            dst = pieces(n, c, me, 1) if n < 2 else slot(n, y)
            remote(source(n, 0), dst, sc_send.at[n, 0], sc_recv.at[n], 0, 0, c, y).wait_recv()

    def y_copy(n, k):
        return remote(slot(n, y), slot(n, y), y_send.at[n, k], y_recv.at[n, y], x, z, c, lax.rem(y + k, 4))

    def z_copy(n, k):
        mine = pieces(n, c, me, 1)
        return remote(mine, mine, z_send.at[n, k], z_recv.at[n, z], x, lax.rem(z + k, 8), c, y)

    def z_start(n):
        def go(k, carry):
            z_copy(n, k).start()
            return carry

        lax.fori_loop(1, 8, go, 0)

    def z_wait(n):
        def wait(k, carry):
            peer = lax.rem(z + k, 8)
            place = pieces(n, c, x * 8 + peer, 1)
            remote(place, place, z_send.at[n, 0], z_recv.at[n, peer], x, peer, c, y).wait_recv()
            return carry

        lax.fori_loop(1, 8, wait, 0)

    def group(n, core, g):
        return pieces(n, core, g * 8, 8)

    def half(n, g, h):
        return pieces(n, c, g * 8 + h * 4, 4)

    def x_copy(n, d):
        mine = group(n, c, x)
        return remote(mine, mine, x_send.at[n, d], x_recv.at[n, d], (right, left)[d], z, c, y)

    def x_wait(n, d):
        g = (left, right)[d]
        place = group(n, c, g)
        remote(place, place, x_send.at[n, d], x_recv.at[n, d], g, z, c, y).wait_recv()

    def relay(n, d):
        part = half(n, (left, right)[d], d)
        return remote(part, part, x_send.at[n, 2 + d], x_recv.at[n, 2 + d], (right, left)[d], z, c, y)

    def relay_wait(n, d):
        place = half(n, far, d)
        remote(place, place, x_send.at[n, 2 + d], x_recv.at[n, 2 + d], (left, right)[d], z, c, y).wait_recv()

    order = (x, left, right, far)

    def cross(n, k):
        place = group(n, c, order[k])
        return remote(place, place, d_send.at[n, k], d_recv.at[n, k], x, z, 1 - c, y)

    def stage_1(n):
        scatter_wait(n)
        if n < 2:
            z_start(n)
        else:
            for k in range(1, 4):
                y_copy(n, k).start()

    def stage_y(n):
        for k in range(1, 4):
            peer = lax.rem(y + k, 4)
            place = slot(n, peer)
            remote(place, place, y_send.at[n, 0], y_recv.at[n, peer], x, z, c, peer).wait_recv()
        rows = slice(SLOT[n], SLOT[n] + ROWS[n])
        at = pl.multiple_of(BASE[n] + c * STRIDE[n] + me * ROWS[n], 8)
        so_ref[pl.ds(at, ROWS[n]), :] = (ybuf[0, rows] + ybuf[1, rows]) + (ybuf[2, rows] + ybuf[3, rows])
        z_start(n)

    def stage_2(n):
        z_wait(n)
        for d in range(2):
            x_copy(n, d).start()
        cross(n, 0).start()

    def stage_3(n):
        for d in range(2):
            x_wait(n, d)
            relay(n, d).start()
            cross(n, 1 + d).start()

    def stage_4(n):
        for d in range(2):
            relay_wait(n, d)
        cross(n, 3).start()

    def stage_5(n):
        for k in range(4):
            place = group(n, 1 - c, order[k])
            remote(place, place, d_send.at[n, k], d_recv.at[n, k], x, z, 1 - c, y).wait_recv()


    def update(h):
        for n in range(2):
            at = slice(n * 512 + h * 256, n * 512 + h * 256 + 256)
            th_ref[at, :], tl_ref[at, :] = split(to_ref[at, :])
        for k in (2, 1, 3, 0):
            at = pl.multiple_of(lax.rem(y + k, 4) * B, B)
            mine = split(past_ref[pl.ds(at, B), :])
            for n in range(2):
                top = slice(n * 512 + h * 256, n * 512 + h * 256 + 256)
                part_ref[k, h, :, n * 256 : n * 256 + 256] = dot3(mine, (th_ref[top, :], tl_ref[top, :]))
            if k == 2:
                for d in range(2):
                    reduce_first(h, d).start()
            elif k:
                reduce_own(h, k // 2).start()

    def reduce_first(h, d):
        return remote(
            part_ref.at[2, h, pl.ds(d * 64, 64)], half_ref.at[h, d], r_send.at[h, d], r_recv.at[h, d],
            x, z, c, (up, down)[d],
        )

    def reduce_own(h, d):
        rows = pl.ds(64 - d * 64, 64)
        return remote(
            part_ref.at[1 + 2 * d, h, rows], full_ref.at[h, d, rows], r_send.at[h, 2 + d], r_recv.at[h, 2 + d],
            x, z, c, (up, down)[d],
        )

    def reduce_sum(h, d):
        rows = pl.ds(d * 64, 64)
        return remote(
            part_ref.at[1 + 2 * d, h, rows], full_ref.at[h, d, rows], r_send.at[h, 4 + d], r_recv.at[h, 4 + d],
            x, z, c, (up, down)[d],
        )

    def update_2(h):
        for d in range(2):
            reduce_first(h, d).wait_recv()
            rows = slice(d * 64, d * 64 + 64)
            part_ref[1 + 2 * d, h, rows, :] += half_ref[h, d]
            reduce_sum(h, d).start()

    def gather(h, d):
        to = pl.ds((1 + 2 * d) * B, B)
        return remote(
            u_ref.at[h, pl.ds(0, B)], u_ref.at[h, to], g_send.at[h, d], g_recv.at[h, d], x, z, c, (up, down)[d]
        )

    def gather_on(h, d):
        mine = pl.ds((1 + 2 * d) * B + d * 64, 64)
        to = pl.ds(2 * B + d * 64, 64)
        return remote(
            u_ref.at[h, mine], u_ref.at[h, to], g_send.at[h, 2 + d], g_recv.at[h, 2 + d], x, z, c, (up, down)[d]
        )

    def update_3(h):
        for d in range(2):
            reduce_own(h, d).wait_recv()
            reduce_sum(h, d).wait_recv()
        at = pl.multiple_of(y * B, B)
        for n in range(2):
            cols = slice(n * 256, n * 256 + 256)
            mat = a_ref[pl.ds(at, B), n * 512 + h * 256 : n * 512 + h * 256 + 256]
            u_ref[h, 0:B, cols] = mat - (part_ref[0, h, :, cols] + (full_ref[h, 0, :, cols] + full_ref[h, 1, :, cols]))
        for d in range(2):
            gather(h, d).start()

    def update_4(h):
        for d in range(2):
            gather(h, d).wait_recv()
            gather_on(h, d).start()

    def update_5(h):
        for d in range(2):
            gather_on(h, d).wait_recv()

    def take(part):
        for core in range(2):
            at = BASE[2 + part] + core * STRIDE[2 + part]
            for n, (i, j) in enumerate(TILES[part][core]):
                top_ref[i * B : i * B + B, j * B : j * B + B] += so_ref[at + n * B : at + n * B + B, :]


    trade = remote(past_ref, other_ref, swap.at[0], swap.at[1], x, z, 1 - c, y)
    trade_a = remote(a_ref.at[:, pl.ds(512, 512)], other_a_ref, swap.at[2], swap.at[3], x, z, 1 - c, y)

    @pl.when(root)
    def _():
        trade.start()
        trade_a.start()
        scatter_all(0)
        z_start(0)
        scatter_all(1)
        z_start(1)
        mine = pl.ds(pl.multiple_of(c * 512, 512), 512)
        theirs = pl.ds(pl.multiple_of(512 - c * 512, 512), 512)
        th_ref[mine, :], tl_ref[mine, :] = split(past_ref[...])
        trade.wait_recv()
        th_ref[theirs, :], tl_ref[theirs, :] = split(other_ref[...])
        trade_a.wait_recv()
        for part in range(3):
            for core in range(2):
                @pl.when(c == core)
                def _(part=part, core=core):
                    top_tiles(part, core, y == 0, th_ref, tl_ref, a_ref, other_a_ref, tiles_ref)

            scatter_all(2 + part)

    @pl.when(jnp.logical_not(root))
    def _():
        for i in range(NBLK):
            top_ref[i * B : i * B + B, 0 : i * B + B] = jnp.zeros((B, i * B + B), f32)
        stage_1(0)
        stage_1(1)

    @pl.when(root)
    def _():
        for i in range(NBLK):
            top_ref[i * B : i * B + B, 0 : i * B + B] = jnp.zeros((B, i * B + B), f32)

    rows_0, rows_1, tiles_a, tiles_b, tiles_c = range(5)
    stage_2(rows_0)
    stage_1(tiles_a)
    stage_2(rows_1)
    stage_y(tiles_a)
    stage_3(rows_0)
    stage_1(tiles_b)
    stage_4(rows_0)
    stage_y(tiles_b)
    stage_2(tiles_a)
    stage_3(rows_1)
    stage_5(rows_0)
    update(0)
    stage_1(tiles_c)
    stage_3(tiles_a)
    stage_4(rows_1)
    stage_2(tiles_b)
    stage_y(tiles_c)
    stage_4(tiles_a)
    stage_5(rows_1)
    update(1)
    stage_5(tiles_a)
    take(0)

    def stage_5b():
        stage_5(tiles_b)
        take(1)

    def stage_5c():
        stage_5(tiles_c)
        take(2)

    events = {
        (0, 1): (lambda: update_2(0),),
        (0, 3): (lambda: stage_3(tiles_b),),
        (0, 7): (lambda: stage_4(tiles_b),),
        (1, -1): (stage_5b,),
        (1, 2): (lambda: stage_2(tiles_c),),
        (1, 4): (lambda: update_2(1),),
        (2, 1): (lambda: stage_3(tiles_c),),
        (2, 5): (lambda: update_3(0),),
        (2, 7): (lambda: stage_4(tiles_c),),
        (3, 0): (stage_5c,),
        (4, 3): (lambda: update_3(1),),
        (4, 6): (lambda: update_4(0),),
        (6, 4): (lambda: update_4(1),),
    }
    factor_top(lh_ref, ll_ref, dh_ref, dl_ref, top_ref, events)
    update_5(0)
    update_5(1)
    solve(y, (x * 16 + z * 2 + c) * 512, u_ref, lh_ref, ll_ref, dh_ref, dl_ref, out_ref, xh_ref, xl_ref)


    @pl.when(root)
    def _():
        trade.wait_send()
        trade_a.wait_send()

        def done(q, carry):
            for n in range(5):
                scatter(n, q).wait_send()
            return carry

        lax.fori_loop(1, 32, done, 0)

    def done_z(k, carry):
        for n in range(5):
            z_copy(n, k).wait_send()
        return carry

    lax.fori_loop(1, 8, done_z, 0)
    for n in range(5):
        if n >= 2:
            for k in range(1, 4):
                y_copy(n, k).wait_send()
        for d in range(2):
            x_copy(n, d).wait_send()
            relay(n, d).wait_send()
        for k in range(4):
            cross(n, k).wait_send()
    for h in range(2):
        for d in range(2):
            reduce_first(h, d).wait_send()
            reduce_own(h, d).wait_send()
            reduce_sum(h, d).wait_send()
            gather(h, d).wait_send()
            gather_on(h, d).wait_send()


def inverse_factor(w, fill):
    lane = lax.broadcasted_iota(jnp.int32, (B, B), 1)
    sub = lax.broadcasted_iota(jnp.int32, (B, B), 0)
    k = PANEL
    at = sub[:k]
    done = []
    for t in range(B // k):
        r0 = t * k
        left = B - r0
        cols = [jnp.broadcast_to(w[:, r0 + m : r0 + m + 1], (left, B)) for m in range(k)]
        lanes, subs = lane[:left], sub[:left]
        unit = jnp.where((lanes == subs + r0) & (subs < k), 1.0, 0.0)
        w = jnp.where((lanes >= r0) & (lanes < r0 + k), unit, w)
        rows = w[:k]
        piv = jnp.stack([col[:k] for col in cols])
        final = jnp.zeros((k, B), f32)
        for m in range(k):
            mine, rest = piv[0], piv[1:]
            inv = lax.rsqrt(jnp.broadcast_to(mine[m : m + 1], (k, B)))
            inv2 = inv * inv
            row = jnp.broadcast_to(rows[m : m + 1], (k, B))
            here = at == m
            final = jnp.where(here, row * inv, final)
            step = row * inv2
            rows = jnp.where(here, step, rows - mine * step)
            if m + 1 < k:
                f = jnp.broadcast_to(rest[:, m : m + 1], (k - 1 - m, k, B)) * inv2[None]
                piv = jnp.where(here[None], f, rest - mine[None] * f)
        done.append(jnp.where(lane[:k] <= at + r0, final, 0.0))
        if left > k:
            w = w[k:]
            for m in range(k):
                w = w - cols[m][k:] * jnp.broadcast_to(rows[m : m + 1], (left - k, B))
        fill(t)
    return jnp.concatenate(done, axis=0)


def factor_top(lh_ref, ll_ref, dh_ref, dl_ref, a_ref, events):
    def rows(i, n=1):
        return slice(i * B, (i + n) * B)

    def low(i, n, j):
        return lh_ref[rows(i, n), rows(j)], ll_ref[rows(i, n), rows(j)]

    def panel(i, n, s, d):
        high, lo = split(dot3(split(a_ref[rows(i, n), rows(s)]), d))
        lh_ref[rows(i, n), rows(s)] = high
        ll_ref[rows(i, n), rows(s)] = lo

    def trail(i, n, j, nj, s):
        a_ref[rows(i, n), rows(j, nj)] -= dot3(low(i, n, s), low(j, nj, s))

    waiting = []
    halves = [None, None]
    for s in range(NBLK):
        def fill(t, s=s):
            for event in events.get((s, t), ()):
                event()
            n = -(-len(waiting) // (B // PANEL - t))
            for _ in range(n):
                waiting.pop(0)()

        for event in events.get((s, -1), ()):
            event()
        d = split(inverse_factor(a_ref[rows(s), rows(s)], fill))
        halves[s % 2] = d
        at = (s % 2) * B
        dh_ref[s // 2, at : at + B, at : at + B] = d[0]
        dl_ref[s // 2, at : at + B, at : at + B] = d[1]
        if s % 2 == 0:
            dh_ref[s // 2, 0:B, B : 2 * B] = jnp.zeros((B, B), bf16)
            dl_ref[s // 2, 0:B, B : 2 * B] = jnp.zeros((B, B), bf16)
        if s + 1 < NBLK:
            panel(s + 1, 1, s, d)
            trail(s + 1, 1, s + 1, 1, s)
        if s + 2 < NBLK:
            def rest(s=s, d=d):
                panel(s + 2, NBLK - s - 2, s, d)

            waiting.append(rest)
            waiting.append(functools.partial(trail, s + 2, NBLK - s - 2, s + 1, 1, s))
            for j in range(s + 2, NBLK):
                waiting.append(functools.partial(trail, j, NBLK - j, j, 1, s))
        if s % 2 == 1:
            def corner(s=s, first=halves[0], second=halves[1]):
                mid = dot3(low(s, 1, s - 1), first, NN)
                high, lo = split(-dot3(second, split(mid), NN))
                dh_ref[s // 2, B : 2 * B, 0:B] = high
                dl_ref[s // 2, B : 2 * B, 0:B] = lo

            waiting.append(corner)
    for job in waiting:
        job()


def solve(depth, base, u_ref, lh_ref, ll_ref, dh_ref, dl_ref, out_ref, xh, xl):
    for n in range(4):
        cols = slice(n * 256, n * 256 + 256)
        u = u_ref[n % 2, :, (n // 2) * 256 : (n // 2) * 256 + 256]
        if n:
            done = slice(0, n * 256)
            u = u - dot3((xh[:, done], xl[:, done]), (lh_ref[cols, done], ll_ref[cols, done]))
        out = dot3(split(u), (dh_ref[n], dl_ref[n]))
        xh[:, cols], xl[:, cols] = split(out)
        col = lax.broadcasted_iota(jnp.int32, (B, 256), 1) + n * 256
        for q in range(4):
            place = pl.multiple_of(lax.rem(depth + 4 - q, 4) * B, B)
            row = lax.broadcasted_iota(jnp.int32, (B, 256), 0) + (base + place)
            out_ref[pl.ds(place, B), cols] = jnp.where(row >= col, out[q * B : q * B + B, :], 0.0)


def body(a_cols, past):
    dma = pltpu.SemaphoreType.DMA
    vmem = pltpu.VMEM
    return pl.pallas_call(
        whole_kernel,
        out_shape=jax.ShapeDtypeStruct((512, W), f32),
        in_specs=[VMEM] * 2,
        out_specs=VMEM,
        scratch_shapes=[
            vmem((36 * B, B), f32),
            vmem((2, 4 * B, 512), f32),
            vmem((W, W), f32),
            vmem((W, W), bf16),
            vmem((W, W), bf16),
            vmem((4, 256, 256), bf16),
            vmem((4, 256, 256), bf16),
            vmem((4 * B, W), bf16),
            vmem((4 * B, W), bf16),
            vmem((W, 512), f32),
            vmem((512, 512), f32),
            vmem((512, 512), f32),
            vmem((18 * B, B), f32),
            vmem((4, 72, B), f32),
            vmem((W, 512), bf16),
            vmem((W, 512), bf16),
            vmem((4, 2, B, 512), f32),
            vmem((2, 2, 64, 512), f32),
            vmem((2, 2, B, 512), f32),
            dma((5, 32)), dma((5,)), dma((5, 4)), dma((5, 4)), dma((5, 8)), dma((5, 8)),
            dma((5, 4)), dma((5, 4)), dma((5, 4)), dma((5, 4)),
            dma((2, 6)), dma((2, 6)), dma((2, 4)), dma((2, 4)), dma((5,)), dma((4,)),
        ],
        compiler_params=pltpu.CompilerParams(collective_id=0, has_side_effects=True),
        name="whole",
    )(past, a_cols)


def solution(mesh):
    split_mesh = Mesh(
        mesh.devices.reshape(mesh.shape["row"], 8, 2, mesh.shape["depth"]), AXES
    )
    placed = (P(ROW_COL, None), P(ROW_COL, "depth"))
    return jax.shard_map(
        body, mesh=split_mesh, in_specs=placed, out_specs=P(ROW_COL, None), check_vma=False
    )
```

```python
import functools

import jax
import jax.numpy as jnp
from jax import lax
from jax.experimental import pallas as pl
from jax.experimental.pallas import tpu as pltpu
from jax.sharding import Mesh
from jax.sharding import PartitionSpec as P

W = 1024
B = 128
NBLK = W // B
PANEL = 16
AXES = ("row", "col_0", "col_1", "depth")
ROW_COL = ("row", "col_0", "col_1")
NT = (((1,), (1,)), ((), ()))
NN = (((1,), (0,)), ((), ()))
f32 = jnp.float32
bf16 = jnp.bfloat16
MESH = pl.DeviceIdType.MESH
VMEM = pl.BlockSpec(memory_space=pltpu.VMEM)


TILES = (
    (((0, 0), (1, 0), (2, 0), (3, 0)), ((4, 0), (5, 0), (6, 0), (7, 0))),
    (
        ((1, 1), (2, 1), (3, 1), (2, 2), (3, 2), (3, 3)),
        ((4, 1), (5, 1), (6, 1), (7, 1), (4, 2), (5, 2)),
    ),
    (
        ((6, 2), (7, 2), (4, 3), (5, 3), (6, 3), (7, 3), (4, 4), (5, 4)),
        ((6, 4), (7, 4), (5, 5), (6, 5), (7, 5), (6, 6), (7, 6), (7, 7)),
    ),
)
ROWS = (8, 8, 16, 24, 32)
BASE = (0, 256, 0, 1024, 2560)
STRIDE = (512, 512, 512, 768, 1024)
SOURCE = (0, 256, 0, 512, 1280)
SLOT = (0, 0, 0, 16, 40)


def split(x):
    high = x.astype(bf16)
    return high, (x - high.astype(f32)).astype(bf16)


def dot3(a, b, dims=NT):
    dot = functools.partial(
        lax.dot_general, dimension_numbers=dims, preferred_element_type=f32
    )
    return dot(a[0], b[0]) + (dot(a[0], b[1]) + dot(a[1], b[0]))


def top_tiles(part, core, first, th_ref, tl_ref, a_ref, other_a_ref, tiles_ref):
    out = SOURCE[2 + part]

    def blocks(i, n=1):
        return slice(i * B, (i + n) * B)

    def value(i, j):
        if core == 1:
            return a_ref[blocks(i - 4), blocks(j)]
        if i < 4:
            return a_ref[blocks(i), blocks(j)]
        if j < 4:
            return a_ref[blocks(j), blocks(i)].T
        return other_a_ref[blocks(i - 4), blocks(j - 4)]

    todo = list(TILES[part][core])
    while todo:
        i, j = todo[0]
        n = 1
        while n < len(todo) and todo[n] == (i + n, j):
            n += 1
        todo = todo[n:]
        product = dot3(
            (th_ref[blocks(i, n), :], tl_ref[blocks(i, n), :]),
            (th_ref[blocks(j), :], tl_ref[blocks(j), :]),
        )
        for k in range(n):
            tiles_ref[out : out + B, :] = jnp.where(first, value(i + k, j), 0.0) - product[blocks(k)]
            out += B


def whole_kernel(
    past_in, a_in, out_ref,
    past_ref, a_ref, perm_ref, so_ref, u_ref, top_ref, lh_ref, ll_ref, dh_ref, dl_ref, xh_ref, xl_ref,
    to_ref, other_ref, other_a_ref, tiles_ref, ybuf, th_ref, tl_ref, part_ref, half_ref, full_ref, bun_t, bun_s,
    sc_send, sc_recv, bu_recv, fw_send, y_send, y_recv, z_send, z_recv, x_send, x_recv, d_send, d_recv,
    r_send, r_recv, g_send, g_recv, loc, swap,
):
    x = lax.axis_index("row")
    z = lax.axis_index("col_0")
    c = lax.axis_index("col_1")
    y = lax.axis_index("depth")
    me = x * 8 + z
    left = lax.rem(x + 3, 4)
    right = lax.rem(x + 1, 4)
    far = lax.rem(x + 2, 4)
    down = lax.rem(y + 3, 4)
    up = lax.rem(y + 1, 4)
    root = me == 0
    load = (
        pltpu.make_async_copy(past_in, past_ref, loc.at[5]),
        pltpu.make_async_copy(a_in, a_ref, loc.at[6]),
    )
    for copy in load:
        copy.start()
    barrier = pltpu.get_barrier_semaphore()

    def greet(*device):
        pl.semaphore_signal(barrier, inc=1, device_id=device, device_id_type=MESH)

    def z_greet(k, carry):
        greet(x, lax.rem(z + k, 8), c, y)
        return carry

    lax.fori_loop(1, 8, z_greet, 0)
    for k in range(1, 4):
        greet(x, z, c, lax.rem(y + k, 4))
    for k in range(1, 4):
        greet(lax.rem(x + k, 4), z, c, y)
    greet(x, z, 1 - c, y)

    for copy in load:
        copy.wait()
    for h in range(2):
        for q in range(32):
            to = (h * 32 + q % 8 * 4 + q // 8) * 8
            perm_ref[to : to + 8, :] = past_ref[(h * 32 + q) * 8 : (h * 32 + q) * 8 + 8, :]
    pl.semaphore_wait(barrier, 14)

    def remote(src, dst, send, recv, *device):
        return pltpu.make_async_remote_copy(
            src_ref=src, dst_ref=dst, send_sem=send, recv_sem=recv,
            device_id=device, device_id_type=MESH,
        )


    def pieces(n, core, start, count):
        at = pl.multiple_of(BASE[n] + core * STRIDE[n] + start * ROWS[n], 8)
        return (to_ref if n < 2 else so_ref).at[pl.ds(at, count * ROWS[n])]

    def slot(n, layer):
        return ybuf.at[layer, pl.ds(SLOT[n], ROWS[n])]


    def source(n, start, count):
        at = pl.multiple_of(SOURCE[n] + start * ROWS[n], 8)
        return (perm_ref if n < 2 else tiles_ref).at[pl.ds(at, count * ROWS[n])]

    def width(n):
        return 4 if n < 2 else 8

    def place_of(n, q):
        return pieces(n, c, q, 1) if n < 2 else slot(n, y)

    def bundle(n, start, count):
        ref, at = (bun_t, n * 32) if n < 2 else (bun_s, 8 * SLOT[n])
        return ref.at[pl.ds(at + start * ROWS[n], count * ROWS[n])]

    def column(n, to):
        place = (0, to) if n < 2 else (to, 0)
        src = source(n, to * width(n), width(n))
        return remote(src, bundle(n, 0, width(n)), sc_send.at[n, to], bu_recv.at[n], *place, c, y)

    def columns_all(n):
        def go(to, carry):
            column(n, to).start()
            return carry

        lax.fori_loop(1, 8 if n < 2 else 4, go, 0)

    def first_piece(n, on_root, k):
        return source(n, k, 1) if on_root else bundle(n, k, 1)

    def onward(n, on_root, k):
        place = (k, z) if n < 2 else (x, k)
        dst = place_of(n, place[0] * 8 + place[1])
        return remote(first_piece(n, on_root, k), dst, fw_send.at[n, k], sc_recv.at[n], *place, c, y)

    def hub(n):
        return jnp.logical_and(x == 0 if n < 2 else z == 0, jnp.logical_not(root))

    def pass_on(n, on_root):
        own = pltpu.make_async_copy(first_piece(n, on_root, 0), place_of(n, me), loc.at[n])
        own.start()
        for k in range(1, width(n)):
            onward(n, on_root, k).start()
        own.wait()

    def stage_h(n):
        @pl.when(hub(n))
        def _():
            whole = bundle(n, 0, width(n))
            remote(whole, whole, sc_send.at[n, 0], bu_recv.at[n], 0, 0, c, y).wait_recv()
            pass_on(n, False)
            send_piece(n)

    def y_copy(n, k):
        return remote(slot(n, y), slot(n, y), y_send.at[n, k], y_recv.at[n, y], x, z, c, lax.rem(y + k, 4))

    def z_copy(n, k):
        mine = pieces(n, c, me, 1)
        return remote(mine, mine, z_send.at[n, k], z_recv.at[n, z], x, lax.rem(z + k, 8), c, y)

    def z_start(n):
        def go(k, carry):
            z_copy(n, k).start()
            return carry

        lax.fori_loop(1, 8, go, 0)

    def z_wait(n):
        def wait(k, carry):
            peer = lax.rem(z + k, 8)
            place = pieces(n, c, x * 8 + peer, 1)
            remote(place, place, z_send.at[n, 0], z_recv.at[n, peer], x, peer, c, y).wait_recv()
            return carry

        lax.fori_loop(1, 8, wait, 0)

    def group(n, core, g):
        return pieces(n, core, g * 8, 8)

    def half(n, g, h):
        return pieces(n, c, g * 8 + h * 4, 4)

    def x_copy(n, d):
        mine = group(n, c, x)
        return remote(mine, mine, x_send.at[n, d], x_recv.at[n, d], (right, left)[d], z, c, y)

    def x_wait(n, d):
        g = (left, right)[d]
        place = group(n, c, g)
        remote(place, place, x_send.at[n, d], x_recv.at[n, d], g, z, c, y).wait_recv()

    def relay(n, d):
        part = half(n, (left, right)[d], d)
        return remote(part, part, x_send.at[n, 2 + d], x_recv.at[n, 2 + d], (right, left)[d], z, c, y)

    def relay_wait(n, d):
        place = half(n, far, d)
        remote(place, place, x_send.at[n, 2 + d], x_recv.at[n, 2 + d], (left, right)[d], z, c, y).wait_recv()

    order = (x, left, right, far)

    def cross(n, k):
        place = group(n, c, order[k])
        return remote(place, place, d_send.at[n, k], d_recv.at[n, k], x, z, 1 - c, y)

    def send_piece(n):
        if n < 2:
            z_start(n)
        else:
            for k in range(1, 4):
                y_copy(n, k).start()

    def stage_0(n):
        columns_all(n)
        pass_on(n, True)
        send_piece(n)

    def stage_1(n):
        @pl.when(x != 0 if n < 2 else z != 0)
        def _():
            place = place_of(n, me)
            remote(place, place, sc_send.at[n, 0], sc_recv.at[n], 0, z, c, y).wait_recv()
            send_piece(n)

    def stage_y(n):
        for k in range(1, 4):
            peer = lax.rem(y + k, 4)
            place = slot(n, peer)
            remote(place, place, y_send.at[n, 0], y_recv.at[n, peer], x, z, c, peer).wait_recv()
        rows = slice(SLOT[n], SLOT[n] + ROWS[n])
        at = pl.multiple_of(BASE[n] + c * STRIDE[n] + me * ROWS[n], 8)
        so_ref[pl.ds(at, ROWS[n]), :] = (ybuf[0, rows] + ybuf[1, rows]) + (ybuf[2, rows] + ybuf[3, rows])
        z_start(n)

    def stage_2(n):
        z_wait(n)
        cross(n, 0).start()
        for d in range(2):
            x_copy(n, d).start()

    def stage_3(n):
        for d in range(2):
            x_wait(n, d)
            cross(n, 1 + d).start()
            relay(n, d).start()

    def stage_4(n):
        for d in range(2):
            relay_wait(n, d)
        cross(n, 3).start()

    def stage_5(n):
        for k in range(4):
            place = group(n, 1 - c, order[k])
            remote(place, place, d_send.at[n, k], d_recv.at[n, k], x, z, 1 - c, y).wait_recv()


    def update(h):
        for n in range(2):
            at = slice(n * 512 + h * 256, n * 512 + h * 256 + 256)
            th_ref[at, :], tl_ref[at, :] = split(to_ref[at, :])
        for k in (2, 1, 3, 0):
            at = pl.multiple_of(lax.rem(y + k, 4) * B, B)
            mine = split(past_ref[pl.ds(at, B), :])
            for n in range(2):
                top = slice(n * 512 + h * 256, n * 512 + h * 256 + 256)
                part_ref[k, h, :, n * 256 : n * 256 + 256] = dot3(mine, (th_ref[top, :], tl_ref[top, :]))
            if k == 2:
                for d in range(2):
                    reduce_first(h, d).start()
            elif k:
                reduce_own(h, k // 2).start()

    def reduce_first(h, d):
        return remote(
            part_ref.at[2, h, pl.ds(d * 64, 64)], half_ref.at[h, d], r_send.at[h, d], r_recv.at[h, d],
            x, z, c, (up, down)[d],
        )

    def reduce_own(h, d):
        rows = pl.ds(64 - d * 64, 64)
        return remote(
            part_ref.at[1 + 2 * d, h, rows], full_ref.at[h, d, rows], r_send.at[h, 2 + d], r_recv.at[h, 2 + d],
            x, z, c, (up, down)[d],
        )

    def reduce_sum(h, d):
        rows = pl.ds(d * 64, 64)
        return remote(
            part_ref.at[1 + 2 * d, h, rows], full_ref.at[h, d, rows], r_send.at[h, 4 + d], r_recv.at[h, 4 + d],
            x, z, c, (up, down)[d],
        )

    def update_2(h):
        for d in range(2):
            reduce_first(h, d).wait_recv()
            rows = slice(d * 64, d * 64 + 64)
            part_ref[1 + 2 * d, h, rows, :] += half_ref[h, d]
            reduce_sum(h, d).start()

    def gather(h, d):
        to = pl.ds((1 + 2 * d) * B, B)
        return remote(
            u_ref.at[h, pl.ds(0, B)], u_ref.at[h, to], g_send.at[h, d], g_recv.at[h, d], x, z, c, (up, down)[d]
        )

    def gather_on(h, d):
        mine = pl.ds((1 + 2 * d) * B + d * 64, 64)
        to = pl.ds(2 * B + d * 64, 64)
        return remote(
            u_ref.at[h, mine], u_ref.at[h, to], g_send.at[h, 2 + d], g_recv.at[h, 2 + d], x, z, c, (up, down)[d]
        )

    def update_3(h):
        for d in range(2):
            reduce_own(h, d).wait_recv()
            reduce_sum(h, d).wait_recv()
        at = pl.multiple_of(y * B, B)
        for n in range(2):
            cols = slice(n * 256, n * 256 + 256)
            mat = a_ref[pl.ds(at, B), n * 512 + h * 256 : n * 512 + h * 256 + 256]
            u_ref[h, 0:B, cols] = mat - (part_ref[0, h, :, cols] + (full_ref[h, 0, :, cols] + full_ref[h, 1, :, cols]))
        for d in range(2):
            gather(h, d).start()

    def update_4(h):
        for d in range(2):
            gather(h, d).wait_recv()
            gather_on(h, d).start()

    def update_5(h):
        for d in range(2):
            gather_on(h, d).wait_recv()

    def take(part):
        for core in range(2):
            at = BASE[2 + part] + core * STRIDE[2 + part]
            for n, (i, j) in enumerate(TILES[part][core]):
                top_ref[i * B : i * B + B, j * B : j * B + B] += so_ref[at + n * B : at + n * B + B, :]


    trade = remote(past_ref, other_ref, swap.at[0], swap.at[1], x, z, 1 - c, y)
    trade_a = remote(a_ref.at[:, pl.ds(512, 512)], other_a_ref, swap.at[2], swap.at[3], x, z, 1 - c, y)

    @pl.when(root)
    def _():
        trade.start()
        trade_a.start()
        stage_0(0)
        stage_0(1)
        mine = pl.ds(pl.multiple_of(c * 512, 512), 512)
        theirs = pl.ds(pl.multiple_of(512 - c * 512, 512), 512)
        th_ref[mine, :], tl_ref[mine, :] = split(past_ref[...])
        trade.wait_recv()
        th_ref[theirs, :], tl_ref[theirs, :] = split(other_ref[...])
        trade_a.wait_recv()
        for part in range(3):
            for core in range(2):
                @pl.when(c == core)
                def _(part=part, core=core):
                    top_tiles(part, core, y == 0, th_ref, tl_ref, a_ref, other_a_ref, tiles_ref)

        stage_0(2)

    rows_0, rows_1, tiles_a, tiles_b, tiles_c = range(5)

    for i in range(NBLK):
        top_ref[i * B : i * B + B, 0 : i * B + B] = jnp.zeros((B, i * B + B), f32)

    def next_part(n):
        @pl.when(root)
        def _():
            stage_0(n)

    def next_part(n):
        @pl.when(root)
        def _():
            stage_0(n)

    stage_h(rows_0)
    stage_1(rows_0)
    stage_h(tiles_a)
    stage_h(rows_1)
    stage_2(rows_0)
    next_part(tiles_b)
    stage_1(rows_1)
    stage_1(tiles_a)
    stage_3(rows_0)
    stage_y(tiles_a)
    stage_4(rows_0)
    stage_h(tiles_b)
    stage_2(rows_1)
    next_part(tiles_c)
    stage_5(rows_0)
    update(0)
    stage_2(tiles_a)
    stage_1(tiles_b)
    stage_3(rows_1)
    stage_3(tiles_a)
    stage_y(tiles_b)
    stage_h(tiles_c)
    stage_4(rows_1)
    stage_4(tiles_a)
    update_2(0)
    stage_5(rows_1)
    stage_2(tiles_b)
    stage_1(tiles_c)
    update(1)
    stage_5(tiles_a)
    take(0)

    def stage_5b():
        stage_5(tiles_b)
        take(1)

    def stage_5c():
        stage_5(tiles_c)
        take(2)

    finish = functools.partial(
        solve, y, u_ref, lh_ref, ll_ref, dh_ref, dl_ref, out_ref, xh_ref, xl_ref
    )

    def update_5ab():
        update_5(0)
        update_5(1)

    events = {
        (0, 0): lambda: stage_3(tiles_b),
        (0, 1): lambda: stage_y(tiles_c),
        (0, 4): lambda: stage_4(tiles_b),
        (0, 6): lambda: update_2(1),
        (1, -1): stage_5b,
        (1, 1): lambda: stage_2(tiles_c),
        (1, 3): lambda: update_3(0),
        (1, 7): lambda: stage_3(tiles_c),
        (2, 4): lambda: update_3(1),
        (2, 7): lambda: stage_4(tiles_c),
        (3, 0): stage_5c,
        (3, 6): lambda: update_4(0),
        (5, 1): lambda: update_4(1),
        (6, 5): update_5ab,
        (7, 0): lambda: finish(0),
        (7, 2): lambda: finish(1),
        (7, 4): lambda: finish(2),
    }
    factor_top(lh_ref, ll_ref, dh_ref, dl_ref, top_ref, events)
    finish(3)


    @pl.when(root)
    def _():
        trade.wait_send()
        trade_a.wait_send()

        for n in range(5):
            for to in range(1, 8 if n < 2 else 4):
                column(n, to).wait_send()
            for k in range(1, width(n)):
                onward(n, True, k).wait_send()

    for n in range(5):
        @pl.when(hub(n))
        def _(n=n):
            for k in range(1, width(n)):
                onward(n, False, k).wait_send()

    def done_z(k, carry):
        for n in range(5):
            z_copy(n, k).wait_send()
        return carry

    lax.fori_loop(1, 8, done_z, 0)
    for n in range(5):
        if n >= 2:
            for k in range(1, 4):
                y_copy(n, k).wait_send()
        for d in range(2):
            x_copy(n, d).wait_send()
            relay(n, d).wait_send()
        for k in range(4):
            cross(n, k).wait_send()
    for h in range(2):
        for d in range(2):
            reduce_first(h, d).wait_send()
            reduce_own(h, d).wait_send()
            reduce_sum(h, d).wait_send()
            gather(h, d).wait_send()
            gather_on(h, d).wait_send()


def inverse_factor(w, fill):
    lane = lax.broadcasted_iota(jnp.int32, (B, B), 1)
    sub = lax.broadcasted_iota(jnp.int32, (B, B), 0)
    k = PANEL
    at = sub[:k]
    done = []
    for t in range(B // k):
        r0 = t * k
        left = B - r0
        cols = [jnp.broadcast_to(w[:, r0 + m : r0 + m + 1], (left, B)) for m in range(k)]
        lanes, subs = lane[:left], sub[:left]
        unit = jnp.where((lanes == subs + r0) & (subs < k), 1.0, 0.0)
        w = jnp.where((lanes >= r0) & (lanes < r0 + k), unit, w)
        rows = w[:k]
        piv = jnp.stack([col[:k] for col in cols])
        final = jnp.zeros((k, B), f32)
        for m in range(k):
            mine, rest = piv[0], piv[1:]
            inv = lax.rsqrt(jnp.broadcast_to(mine[m : m + 1], (k, B)))
            inv2 = inv * inv
            row = jnp.broadcast_to(rows[m : m + 1], (k, B))
            here = at == m
            final = jnp.where(here, row * inv, final)
            step = row * inv2
            rows = jnp.where(here, step, rows - mine * step)
            if m + 1 < k:
                f = jnp.broadcast_to(rest[:, m : m + 1], (k - 1 - m, k, B)) * inv2[None]
                piv = jnp.where(here[None], f, rest - mine[None] * f)
        done.append(jnp.where(lane[:k] <= at + r0, final, 0.0))
        if left > k:
            w = w[k:]
            for m in range(k):
                w = w - cols[m][k:] * jnp.broadcast_to(rows[m : m + 1], (left - k, B))
        fill(t)
    return jnp.concatenate(done, axis=0)


def factor_top(lh_ref, ll_ref, dh_ref, dl_ref, a_ref, events):
    def rows(i, n=1):
        return slice(i * B, (i + n) * B)

    def low(i, n, j):
        return lh_ref[rows(i, n), rows(j)], ll_ref[rows(i, n), rows(j)]

    def panel(i, n, s, d):
        high, lo = split(dot3(split(a_ref[rows(i, n), rows(s)]), d))
        lh_ref[rows(i, n), rows(s)] = high
        ll_ref[rows(i, n), rows(s)] = lo

    def trail(i, n, j, nj, s):
        a_ref[rows(i, n), rows(j, nj)] -= dot3(low(i, n, s), low(j, nj, s))

    waiting = []
    halves = [None, None]
    for s in range(NBLK):
        def fill(t, s=s):
            if (s, t) in events:
                events[s, t]()
            n = -(-len(waiting) // (B // PANEL - t))
            for _ in range(n):
                waiting.pop(0)()

        if (s, -1) in events:
            events[s, -1]()
        d = split(inverse_factor(a_ref[rows(s), rows(s)], fill))
        halves[s % 2] = d
        at = (s % 2) * B
        dh_ref[s // 2, at : at + B, at : at + B] = d[0]
        dl_ref[s // 2, at : at + B, at : at + B] = d[1]
        if s % 2 == 0:
            dh_ref[s // 2, 0:B, B : 2 * B] = jnp.zeros((B, B), bf16)
            dl_ref[s // 2, 0:B, B : 2 * B] = jnp.zeros((B, B), bf16)
        if s + 1 < NBLK:
            panel(s + 1, 1, s, d)
            trail(s + 1, 1, s + 1, 1, s)
        if s + 2 < NBLK:
            def rest(s=s, d=d):
                panel(s + 2, NBLK - s - 2, s, d)

            waiting.append(rest)
            waiting.append(functools.partial(trail, s + 2, NBLK - s - 2, s + 1, 1, s))
            for j in range(s + 2, NBLK):
                waiting.append(functools.partial(trail, j, NBLK - j, j, 1, s))
        if s % 2 == 1:
            def corner(s=s, first=halves[0], second=halves[1]):
                mid = dot3(low(s, 1, s - 1), first, NN)
                high, lo = split(-dot3(second, split(mid), NN))
                dh_ref[s // 2, B : 2 * B, 0:B] = high
                dl_ref[s // 2, B : 2 * B, 0:B] = lo

            waiting.append(corner)
    for job in waiting:
        job()


def solve(depth, u_ref, lh_ref, ll_ref, dh_ref, dl_ref, out_ref, xh, xl, n):
    cols = slice(n * 256, n * 256 + 256)
    u = u_ref[n % 2, :, (n // 2) * 256 : (n // 2) * 256 + 256]
    if n:
        done = slice(0, n * 256)
        u = u - dot3((xh[:, done], xl[:, done]), (lh_ref[cols, done], ll_ref[cols, done]))
    out = dot3(split(u), (dh_ref[n], dl_ref[n]))
    if n < 3:
        xh[:, cols], xl[:, cols] = split(out)
    for q in range(4):
        place = pl.multiple_of(lax.rem(depth + 4 - q, 4) * B, B)
        out_ref[pl.ds(place, B), cols] = out[q * B : q * B + B, :]


def body(a_cols, past):
    dma = pltpu.SemaphoreType.DMA
    vmem = pltpu.VMEM
    solved = pl.pallas_call(
        whole_kernel,
        out_shape=jax.ShapeDtypeStruct((512, W), f32),
        in_specs=[pl.BlockSpec(memory_space=pltpu.HBM)] * 2,
        out_specs=VMEM,
        scratch_shapes=[
            vmem((512, 512), f32),
            vmem((512, W), f32),
            vmem((512, 512), f32),
            vmem((36 * B, B), f32),
            vmem((2, 4 * B, 512), f32),
            vmem((W, W), f32),
            vmem((W, W), bf16),
            vmem((W, W), bf16),
            vmem((4, 256, 256), bf16),
            vmem((4, 256, 256), bf16),
            vmem((4 * B, W), bf16),
            vmem((4 * B, W), bf16),
            vmem((W, 512), f32),
            vmem((512, 512), f32),
            vmem((512, 512), f32),
            vmem((18 * B, B), f32),
            vmem((4, 72, B), f32),
            vmem((W, 512), bf16),
            vmem((W, 512), bf16),
            vmem((4, 2, B, 512), f32),
            vmem((2, 2, 64, 512), f32),
            vmem((2, 2, B, 512), f32),
            vmem((64, 512), f32),
            vmem((576, B), f32),
            dma((5, 8)), dma((5,)), dma((5,)), dma((5, 8)), dma((5, 4)), dma((5, 4)), dma((5, 8)), dma((5, 8)),
            dma((5, 4)), dma((5, 4)), dma((5, 4)), dma((5, 4)),
            dma((2, 6)), dma((2, 6)), dma((2, 4)), dma((2, 4)), dma((7,)), dma((4,)),
        ],
        compiler_params=pltpu.CompilerParams(collective_id=0, has_side_effects=True, vmem_limit_bytes=40 * 2**20),
        name="whole",
    )(past, a_cols)
    x, z, c = (lax.axis_index(axis) for axis in ROW_COL)
    row = (x * 16 + z * 2 + c) * 512 + lax.broadcasted_iota(jnp.int32, (512, W), 0)
    return jnp.where(row >= lax.broadcasted_iota(jnp.int32, (512, W), 1), solved, 0.0)


def solution(mesh):
    split_mesh = Mesh(
        mesh.devices.reshape(mesh.shape["row"], 8, 2, mesh.shape["depth"]), AXES
    )
    placed = (P(ROW_COL, None), P(ROW_COL, "depth"))
    return jax.shard_map(
        body, mesh=split_mesh, in_specs=placed, out_specs=P(ROW_COL, None), check_vma=False
    )
```

```python
import functools

import jax
import jax.numpy as jnp
from jax import lax
from jax.experimental import pallas as pl
from jax.experimental.pallas import tpu as pltpu
from jax.sharding import Mesh
from jax.sharding import PartitionSpec as P

W = 1024
B = 128
NBLK = W // B
PANEL = 16
AXES = ("row", "col_0", "col_1", "depth")
ROW_COL = ("row", "col_0", "col_1")
NT = (((1,), (1,)), ((), ()))
NN = (((1,), (0,)), ((), ()))
f32 = jnp.float32
bf16 = jnp.bfloat16
MESH = pl.DeviceIdType.MESH
VMEM = pl.BlockSpec(memory_space=pltpu.VMEM)


TILES = (
    (((0, 0), (1, 0), (2, 0), (3, 0)), ((4, 0), (5, 0), (6, 0), (7, 0))),
    (
        ((1, 1), (2, 1), (3, 1), (2, 2), (3, 2), (3, 3)),
        ((4, 1), (5, 1), (6, 1), (7, 1), (4, 2), (5, 2)),
    ),
    (
        ((6, 2), (7, 2), (4, 3), (5, 3), (6, 3), (7, 3), (4, 4), (5, 4)),
        ((6, 4), (7, 4), (5, 5), (6, 5), (7, 5), (6, 6), (7, 6), (7, 7)),
    ),
)
ROWS = (8, 8, 16, 24, 32)
BASE = (0, 256, 0, 1024, 2560)
STRIDE = (512, 512, 512, 768, 1024)
SOURCE = (0, 256, 0, 512, 1280)
SLOT = (0, 0, 0, 16, 40)
FAR_FIRST = (4, 3, 5, 2, 6, 1, 7)


def split(x):
    high = x.astype(bf16)
    return high, (x - high.astype(f32)).astype(bf16)


def dot3(a, b, dims=NT):
    dot = functools.partial(
        lax.dot_general, dimension_numbers=dims, preferred_element_type=f32
    )
    return dot(a[0], b[0]) + (dot(a[0], b[1]) + dot(a[1], b[0]))


def top_tiles(part, core, first, th_ref, tl_ref, a_ref, other_a_ref, tiles_ref):
    out = SOURCE[2 + part]

    def blocks(i, n=1):
        return slice(i * B, (i + n) * B)

    def value(i, j):
        if core == 1:
            return a_ref[blocks(i - 4), blocks(j)]
        if i < 4:
            return a_ref[blocks(i), blocks(j)]
        if j < 4:
            return a_ref[blocks(j), blocks(i)].T
        return other_a_ref[blocks(i - 4), blocks(j - 4)]

    todo = list(TILES[part][core])
    while todo:
        i, j = todo[0]
        n = 1
        while n < len(todo) and todo[n] == (i + n, j):
            n += 1
        todo = todo[n:]
        product = dot3(
            (th_ref[blocks(i, n), :], tl_ref[blocks(i, n), :]),
            (th_ref[blocks(j), :], tl_ref[blocks(j), :]),
        )
        for k in range(n):
            tiles_ref[out : out + B, :] = jnp.where(first, value(i + k, j), 0.0) - product[blocks(k)]
            out += B


def whole_kernel(
    past_in, a_in, out_ref,
    past_ref, a_ref, perm_ref, so_ref, u_ref, top_ref, lh_ref, ll_ref, dh_ref, dl_ref, xh_ref, xl_ref,
    to_ref, other_ref, other_a_ref, tiles_ref, ybuf, th_ref, tl_ref, part_ref, half_ref, full_ref, bun_t, bun_s,
    sc_send, sc_recv, bu_recv, fw_send, y_send, y_recv, z_send, z_recv, x_send, x_recv, d_send, d_recv,
    r_send, r_recv, g_send, g_recv, loc, swap,
):
    x = lax.axis_index("row")
    z = lax.axis_index("col_0")
    c = lax.axis_index("col_1")
    y = lax.axis_index("depth")
    me = x * 8 + z
    left = lax.rem(x + 3, 4)
    right = lax.rem(x + 1, 4)
    far = lax.rem(x + 2, 4)
    down = lax.rem(y + 3, 4)
    up = lax.rem(y + 1, 4)
    root = me == 0
    load = (
        pltpu.make_async_copy(past_in, past_ref, loc.at[5]),
        pltpu.make_async_copy(a_in, a_ref, loc.at[6]),
    )
    for copy in load:
        copy.start()
    barrier = pltpu.get_barrier_semaphore()

    def greet(*device):
        pl.semaphore_signal(barrier, inc=1, device_id=device, device_id_type=MESH)

    def z_greet(k, carry):
        greet(x, lax.rem(z + k, 8), c, y)
        return carry

    lax.fori_loop(1, 8, z_greet, 0)
    for k in range(1, 4):
        greet(x, z, c, lax.rem(y + k, 4))
    for k in range(1, 4):
        greet(lax.rem(x + k, 4), z, c, y)
    greet(x, z, 1 - c, y)

    for copy in load:
        copy.wait()
    for h in range(2):
        for q in range(32):
            to = (h * 32 + q % 8 * 4 + q // 8) * 8
            perm_ref[to : to + 8, :] = past_ref[(h * 32 + q) * 8 : (h * 32 + q) * 8 + 8, :]
    pl.semaphore_wait(barrier, 14)

    def remote(src, dst, send, recv, *device):
        return pltpu.make_async_remote_copy(
            src_ref=src, dst_ref=dst, send_sem=send, recv_sem=recv,
            device_id=device, device_id_type=MESH,
        )


    def pieces(n, core, start, count):
        at = pl.multiple_of(BASE[n] + core * STRIDE[n] + start * ROWS[n], 8)
        return (to_ref if n < 2 else so_ref).at[pl.ds(at, count * ROWS[n])]

    def slot(n, layer):
        return ybuf.at[layer, pl.ds(SLOT[n], ROWS[n])]


    def source(n, start, count):
        at = pl.multiple_of(SOURCE[n] + start * ROWS[n], 8)
        return (perm_ref if n < 2 else tiles_ref).at[pl.ds(at, count * ROWS[n])]

    def width(n):
        return 4 if n < 2 else 8

    def place_of(n, q):
        return pieces(n, c, q, 1) if n < 2 else slot(n, y)

    def bundle(n, start, count):
        ref, at = (bun_t, n * 32) if n < 2 else (bun_s, 8 * SLOT[n])
        return ref.at[pl.ds(at + start * ROWS[n], count * ROWS[n])]

    def column(n, to):
        place = (0, to) if n < 2 else (to, 0)
        src = source(n, to * width(n), width(n))
        return remote(src, bundle(n, 0, width(n)), sc_send.at[n, to], bu_recv.at[n], *place, c, y)

    def columns_all(n):
        for to in FAR_FIRST if n < 2 else (2, 1, 3):
            column(n, to).start()

    def first_piece(n, on_root, k):
        return source(n, k, 1) if on_root else bundle(n, k, 1)

    def onward(n, on_root, k):
        place = (k, z) if n < 2 else (x, k)
        dst = place_of(n, place[0] * 8 + place[1])
        return remote(first_piece(n, on_root, k), dst, fw_send.at[n, k], sc_recv.at[n], *place, c, y)

    def hub(n):
        return jnp.logical_and(x == 0 if n < 2 else z == 0, jnp.logical_not(root))

    def pass_on(n, on_root):
        own = pltpu.make_async_copy(first_piece(n, on_root, 0), place_of(n, me), loc.at[n])
        own.start()
        for k in (2, 1, 3) if n < 2 else FAR_FIRST:
            onward(n, on_root, k).start()
        own.wait()

    def stage_h(n):
        @pl.when(hub(n))
        def _():
            whole = bundle(n, 0, width(n))
            remote(whole, whole, sc_send.at[n, 0], bu_recv.at[n], 0, 0, c, y).wait_recv()
            pass_on(n, False)
            send_piece(n)

    def y_copy(n, k):
        return remote(slot(n, y), slot(n, y), y_send.at[n, k], y_recv.at[n, y], x, z, c, lax.rem(y + k, 4))

    def z_copy(n, k):
        mine = pieces(n, c, me, 1)
        return remote(mine, mine, z_send.at[n, k], z_recv.at[n, z], x, lax.rem(z + k, 8), c, y)

    def z_start(n):
        for k in FAR_FIRST:
            z_copy(n, k).start()

    def z_wait(n):
        def wait(k, carry):
            peer = lax.rem(z + k, 8)
            place = pieces(n, c, x * 8 + peer, 1)
            remote(place, place, z_send.at[n, 0], z_recv.at[n, peer], x, peer, c, y).wait_recv()
            return carry

        lax.fori_loop(1, 8, wait, 0)

    def group(n, core, g):
        return pieces(n, core, g * 8, 8)

    def half(n, g, h):
        return pieces(n, c, g * 8 + h * 4, 4)

    def x_copy(n, d):
        mine = group(n, c, x)
        return remote(mine, mine, x_send.at[n, d], x_recv.at[n, d], (right, left)[d], z, c, y)

    def x_wait(n, d):
        g = (left, right)[d]
        place = group(n, c, g)
        remote(place, place, x_send.at[n, d], x_recv.at[n, d], g, z, c, y).wait_recv()

    def relay(n, d):
        part = half(n, (left, right)[d], d)
        return remote(part, part, x_send.at[n, 2 + d], x_recv.at[n, 2 + d], (right, left)[d], z, c, y)

    def relay_wait(n, d):
        place = half(n, far, d)
        remote(place, place, x_send.at[n, 2 + d], x_recv.at[n, 2 + d], (left, right)[d], z, c, y).wait_recv()

    order = (x, left, right, far)

    def cross(n, k):
        place = group(n, c, order[k])
        return remote(place, place, d_send.at[n, k], d_recv.at[n, k], x, z, 1 - c, y)

    def send_piece(n):
        if n < 2:
            z_start(n)
        else:
            for k in range(1, 4):
                y_copy(n, k).start()

    def stage_0(n):
        columns_all(n)
        pass_on(n, True)
        send_piece(n)

    def stage_1(n):
        @pl.when(x != 0 if n < 2 else z != 0)
        def _():
            place = place_of(n, me)
            remote(place, place, sc_send.at[n, 0], sc_recv.at[n], 0, z, c, y).wait_recv()
            send_piece(n)

    def stage_y(n):
        for k in range(1, 4):
            peer = lax.rem(y + k, 4)
            place = slot(n, peer)
            remote(place, place, y_send.at[n, 0], y_recv.at[n, peer], x, z, c, peer).wait_recv()
        rows = slice(SLOT[n], SLOT[n] + ROWS[n])
        at = pl.multiple_of(BASE[n] + c * STRIDE[n] + me * ROWS[n], 8)
        so_ref[pl.ds(at, ROWS[n]), :] = (ybuf[0, rows] + ybuf[1, rows]) + (ybuf[2, rows] + ybuf[3, rows])
        z_start(n)

    def stage_2(n):
        z_wait(n)
        cross(n, 0).start()
        for d in range(2):
            x_copy(n, d).start()

    def stage_3(n):
        for d in range(2):
            x_wait(n, d)
            cross(n, 1 + d).start()
            relay(n, d).start()

    def stage_4(n):
        for d in range(2):
            relay_wait(n, d)
        cross(n, 3).start()

    def stage_5(n):
        for k in range(4):
            place = group(n, 1 - c, order[k])
            remote(place, place, d_send.at[n, k], d_recv.at[n, k], x, z, 1 - c, y).wait_recv()


    def update(h):
        for n in range(2):
            at = slice(n * 512 + h * 256, n * 512 + h * 256 + 256)
            th_ref[at, :], tl_ref[at, :] = split(to_ref[at, :])
        for k in (2, 1, 3, 0):
            at = pl.multiple_of(lax.rem(y + k, 4) * B, B)
            mine = split(past_ref[pl.ds(at, B), :])
            for n in range(2):
                top = slice(n * 512 + h * 256, n * 512 + h * 256 + 256)
                part_ref[k, h, :, n * 256 : n * 256 + 256] = dot3(mine, (th_ref[top, :], tl_ref[top, :]))
            if k == 2:
                for d in range(2):
                    reduce_first(h, d).start()
            elif k:
                reduce_own(h, k // 2).start()

    def reduce_first(h, d):
        return remote(
            part_ref.at[2, h, pl.ds(d * 64, 64)], half_ref.at[h, d], r_send.at[h, d], r_recv.at[h, d],
            x, z, c, (up, down)[d],
        )

    def reduce_own(h, d):
        rows = pl.ds(64 - d * 64, 64)
        return remote(
            part_ref.at[1 + 2 * d, h, rows], full_ref.at[h, d, rows], r_send.at[h, 2 + d], r_recv.at[h, 2 + d],
            x, z, c, (up, down)[d],
        )

    def reduce_sum(h, d):
        rows = pl.ds(d * 64, 64)
        return remote(
            part_ref.at[1 + 2 * d, h, rows], full_ref.at[h, d, rows], r_send.at[h, 4 + d], r_recv.at[h, 4 + d],
            x, z, c, (up, down)[d],
        )

    def update_2(h):
        for d in range(2):
            reduce_first(h, d).wait_recv()
            rows = slice(d * 64, d * 64 + 64)
            part_ref[1 + 2 * d, h, rows, :] += half_ref[h, d]
            reduce_sum(h, d).start()

    def gather(h, d):
        to = pl.ds((1 + 2 * d) * B, B)
        return remote(
            u_ref.at[h, pl.ds(0, B)], u_ref.at[h, to], g_send.at[h, d], g_recv.at[h, d], x, z, c, (up, down)[d]
        )

    def gather_on(h, d):
        mine = pl.ds((1 + 2 * d) * B + d * 64, 64)
        to = pl.ds(2 * B + d * 64, 64)
        return remote(
            u_ref.at[h, mine], u_ref.at[h, to], g_send.at[h, 2 + d], g_recv.at[h, 2 + d], x, z, c, (up, down)[d]
        )

    def update_3(h):
        for d in range(2):
            reduce_own(h, d).wait_recv()
            reduce_sum(h, d).wait_recv()
        at = pl.multiple_of(y * B, B)
        for n in range(2):
            cols = slice(n * 256, n * 256 + 256)
            mat = a_ref[pl.ds(at, B), n * 512 + h * 256 : n * 512 + h * 256 + 256]
            u_ref[h, 0:B, cols] = mat - (part_ref[0, h, :, cols] + (full_ref[h, 0, :, cols] + full_ref[h, 1, :, cols]))
        for d in range(2):
            gather(h, d).start()

    def update_4(h):
        for d in range(2):
            gather(h, d).wait_recv()
            gather_on(h, d).start()

    def update_5(h):
        for d in range(2):
            gather_on(h, d).wait_recv()

    def take(part):
        for core in range(2):
            at = BASE[2 + part] + core * STRIDE[2 + part]
            for n, (i, j) in enumerate(TILES[part][core]):
                top_ref[i * B : i * B + B, j * B : j * B + B] += so_ref[at + n * B : at + n * B + B, :]


    trade = remote(past_ref, other_ref, swap.at[0], swap.at[1], x, z, 1 - c, y)
    trade_a = remote(a_ref.at[:, pl.ds(512, 512)], other_a_ref, swap.at[2], swap.at[3], x, z, 1 - c, y)

    @pl.when(root)
    def _():
        trade.start()
        trade_a.start()
        stage_0(0)
        stage_0(1)
        mine = pl.ds(pl.multiple_of(c * 512, 512), 512)
        theirs = pl.ds(pl.multiple_of(512 - c * 512, 512), 512)
        th_ref[mine, :], tl_ref[mine, :] = split(past_ref[...])
        trade.wait_recv()
        th_ref[theirs, :], tl_ref[theirs, :] = split(other_ref[...])
        trade_a.wait_recv()
        for part in range(3):
            for core in range(2):
                @pl.when(c == core)
                def _(part=part, core=core):
                    top_tiles(part, core, y == 0, th_ref, tl_ref, a_ref, other_a_ref, tiles_ref)

        stage_0(2)

    rows_0, rows_1, tiles_a, tiles_b, tiles_c = range(5)

    for i in range(NBLK):
        top_ref[i * B : i * B + B, 0 : i * B + B] = jnp.zeros((B, i * B + B), f32)

    def next_part(n):
        @pl.when(root)
        def _():
            stage_0(n)

    def next_part(n):
        @pl.when(root)
        def _():
            stage_0(n)

    stage_h(rows_0)
    stage_1(rows_0)
    stage_h(tiles_a)
    stage_h(rows_1)
    stage_2(rows_0)
    next_part(tiles_b)
    stage_1(rows_1)
    stage_1(tiles_a)
    stage_3(rows_0)
    stage_y(tiles_a)
    stage_4(rows_0)
    stage_h(tiles_b)
    stage_2(rows_1)
    next_part(tiles_c)
    stage_1(tiles_b)
    stage_5(rows_0)
    update(0)
    stage_h(tiles_c)
    stage_2(tiles_a)
    stage_3(rows_1)
    stage_y(tiles_b)
    stage_3(tiles_a)
    stage_4(rows_1)
    stage_1(tiles_c)
    stage_2(tiles_b)
    stage_4(tiles_a)
    update_2(0)
    stage_5(rows_1)
    stage_y(tiles_c)
    update(1)
    stage_3(tiles_b)
    stage_5(tiles_a)
    take(0)

    def stage_5b():
        stage_5(tiles_b)
        take(1)

    def stage_5c():
        stage_5(tiles_c)
        take(2)

    finish = functools.partial(
        solve, y, u_ref, lh_ref, ll_ref, dh_ref, dl_ref, out_ref, xh_ref, xl_ref
    )

    def update_5ab():
        update_5(0)
        update_5(1)

    events = {
        (0, 4): lambda: stage_4(tiles_b),
        (0, 5): lambda: stage_2(tiles_c),
        (0, 6): lambda: update_2(1),
        (0, 7): lambda: update_3(0),
        (1, -1): stage_5b,
        (1, 6): lambda: stage_3(tiles_c),
        (2, 2): lambda: update_3(1),
        (2, 6): lambda: stage_4(tiles_c),
        (3, 2): stage_5c,
        (3, 3): lambda: update_4(0),
        (5, 1): lambda: update_4(1),
        (6, 6): update_5ab,
        (7, 0): lambda: finish(0),
        (7, 2): lambda: finish(1),
        (7, 4): lambda: finish(2),
    }
    factor_top(lh_ref, ll_ref, dh_ref, dl_ref, top_ref, events)
    finish(3)


    @pl.when(root)
    def _():
        trade.wait_send()
        trade_a.wait_send()

        for n in range(5):
            for to in range(1, 8 if n < 2 else 4):
                column(n, to).wait_send()
            for k in range(1, width(n)):
                onward(n, True, k).wait_send()

    for n in range(5):
        @pl.when(hub(n))
        def _(n=n):
            for k in range(1, width(n)):
                onward(n, False, k).wait_send()

    def done_z(k, carry):
        for n in range(5):
            z_copy(n, k).wait_send()
        return carry

    lax.fori_loop(1, 8, done_z, 0)
    for n in range(5):
        if n >= 2:
            for k in range(1, 4):
                y_copy(n, k).wait_send()
        for d in range(2):
            x_copy(n, d).wait_send()
            relay(n, d).wait_send()
        for k in range(4):
            cross(n, k).wait_send()
    for h in range(2):
        for d in range(2):
            reduce_first(h, d).wait_send()
            reduce_own(h, d).wait_send()
            reduce_sum(h, d).wait_send()
            gather(h, d).wait_send()
            gather_on(h, d).wait_send()


def inverse_factor(w, fill):
    lane = lax.broadcasted_iota(jnp.int32, (B, B), 1)
    sub = lax.broadcasted_iota(jnp.int32, (B, B), 0)
    k = PANEL
    at = sub[:k]
    done = []
    for t in range(B // k):
        r0 = t * k
        left = B - r0
        cols = [jnp.broadcast_to(w[:, r0 + m : r0 + m + 1], (left, B)) for m in range(k)]
        lanes, subs = lane[:left], sub[:left]
        unit = jnp.where((lanes == subs + r0) & (subs < k), 1.0, 0.0)
        w = jnp.where((lanes >= r0) & (lanes < r0 + k), unit, w)
        rows = w[:k]
        piv = jnp.stack([col[:k] for col in cols])
        final = jnp.zeros((k, B), f32)
        for m in range(k):
            mine, rest = piv[0], piv[1:]
            inv = lax.rsqrt(jnp.broadcast_to(mine[m : m + 1], (k, B)))
            inv2 = inv * inv
            row = jnp.broadcast_to(rows[m : m + 1], (k, B))
            here = at == m
            final = jnp.where(here, row * inv, final)
            step = row * inv2
            rows = jnp.where(here, step, rows - mine * step)
            if m + 1 < k:
                f = jnp.broadcast_to(rest[:, m : m + 1], (k - 1 - m, k, B)) * inv2[None]
                piv = jnp.where(here[None], f, rest - mine[None] * f)
        done.append(jnp.where(lane[:k] <= at + r0, final, 0.0))
        if left > k:
            w = w[k:]
            for m in range(k):
                w = w - cols[m][k:] * jnp.broadcast_to(rows[m : m + 1], (left - k, B))
        fill(t)
    return jnp.concatenate(done, axis=0)


def factor_top(lh_ref, ll_ref, dh_ref, dl_ref, a_ref, events):
    def rows(i, n=1):
        return slice(i * B, (i + n) * B)

    def low(i, n, j):
        return lh_ref[rows(i, n), rows(j)], ll_ref[rows(i, n), rows(j)]

    def panel(i, n, s, d):
        high, lo = split(dot3(split(a_ref[rows(i, n), rows(s)]), d))
        lh_ref[rows(i, n), rows(s)] = high
        ll_ref[rows(i, n), rows(s)] = lo

    def trail(i, n, j, nj, s):
        a_ref[rows(i, n), rows(j, nj)] -= dot3(low(i, n, s), low(j, nj, s))

    waiting = []
    halves = [None, None]
    for s in range(NBLK):
        def fill(t, s=s):
            if (s, t) in events:
                events[s, t]()
            if s == 3 and t < 2:
                return
            n = -(-len(waiting) // (B // PANEL - t))
            for _ in range(n):
                waiting.pop(0)()

        if (s, -1) in events:
            events[s, -1]()
        d = split(inverse_factor(a_ref[rows(s), rows(s)], fill))
        halves[s % 2] = d
        at = (s % 2) * B
        dh_ref[s // 2, at : at + B, at : at + B] = d[0]
        dl_ref[s // 2, at : at + B, at : at + B] = d[1]
        if s % 2 == 0:
            dh_ref[s // 2, 0:B, B : 2 * B] = jnp.zeros((B, B), bf16)
            dl_ref[s // 2, 0:B, B : 2 * B] = jnp.zeros((B, B), bf16)
        if s + 1 < NBLK:
            panel(s + 1, 1, s, d)
            trail(s + 1, 1, s + 1, 1, s)
        if s + 2 < NBLK:
            def rest(s=s, d=d):
                panel(s + 2, NBLK - s - 2, s, d)

            waiting.append(rest)
            waiting.append(functools.partial(trail, s + 2, NBLK - s - 2, s + 1, 1, s))
            for j in range(s + 2, NBLK):
                waiting.append(functools.partial(trail, j, NBLK - j, j, 1, s))
        if s % 2 == 1:
            def corner(s=s, first=halves[0], second=halves[1]):
                mid = dot3(low(s, 1, s - 1), first, NN)
                high, lo = split(-dot3(second, split(mid), NN))
                dh_ref[s // 2, B : 2 * B, 0:B] = high
                dl_ref[s // 2, B : 2 * B, 0:B] = lo

            waiting.append(corner)
    for job in waiting:
        job()


def solve(depth, u_ref, lh_ref, ll_ref, dh_ref, dl_ref, out_ref, xh, xl, n):
    cols = slice(n * 256, n * 256 + 256)
    u = u_ref[n % 2, :, (n // 2) * 256 : (n // 2) * 256 + 256]
    if n:
        done = slice(0, n * 256)
        u = u - dot3((xh[:, done], xl[:, done]), (lh_ref[cols, done], ll_ref[cols, done]))
    out = dot3(split(u), (dh_ref[n], dl_ref[n]))
    if n < 3:
        xh[:, cols], xl[:, cols] = split(out)
    for q in range(4):
        place = pl.multiple_of(lax.rem(depth + 4 - q, 4) * B, B)
        out_ref[pl.ds(place, B), cols] = out[q * B : q * B + B, :]


def body(a_cols, past):
    dma = pltpu.SemaphoreType.DMA
    vmem = pltpu.VMEM
    solved = pl.pallas_call(
        whole_kernel,
        out_shape=jax.ShapeDtypeStruct((512, W), f32),
        in_specs=[pl.BlockSpec(memory_space=pltpu.HBM)] * 2,
        out_specs=VMEM,
        scratch_shapes=[
            vmem((512, 512), f32),
            vmem((512, W), f32),
            vmem((512, 512), f32),
            vmem((36 * B, B), f32),
            vmem((2, 4 * B, 512), f32),
            vmem((W, W), f32),
            vmem((W, W), bf16),
            vmem((W, W), bf16),
            vmem((4, 256, 256), bf16),
            vmem((4, 256, 256), bf16),
            vmem((4 * B, W), bf16),
            vmem((4 * B, W), bf16),
            vmem((W, 512), f32),
            vmem((512, 512), f32),
            vmem((512, 512), f32),
            vmem((18 * B, B), f32),
            vmem((4, 72, B), f32),
            vmem((W, 512), bf16),
            vmem((W, 512), bf16),
            vmem((4, 2, B, 512), f32),
            vmem((2, 2, 64, 512), f32),
            vmem((2, 2, B, 512), f32),
            vmem((64, 512), f32),
            vmem((576, B), f32),
            dma((5, 8)), dma((5,)), dma((5,)), dma((5, 8)), dma((5, 4)), dma((5, 4)), dma((5, 8)), dma((5, 8)),
            dma((5, 4)), dma((5, 4)), dma((5, 4)), dma((5, 4)),
            dma((2, 6)), dma((2, 6)), dma((2, 4)), dma((2, 4)), dma((7,)), dma((4,)),
        ],
        compiler_params=pltpu.CompilerParams(collective_id=0, has_side_effects=True, vmem_limit_bytes=40 * 2**20),
        name="whole",
    )(past, a_cols)
    x, z, c = (lax.axis_index(axis) for axis in ROW_COL)
    row = (x * 16 + z * 2 + c) * 512 + lax.broadcasted_iota(jnp.int32, (512, W), 0)
    return jnp.where(row >= lax.broadcasted_iota(jnp.int32, (512, W), 1), solved, 0.0)


def solution(mesh):
    split_mesh = Mesh(
        mesh.devices.reshape(mesh.shape["row"], 8, 2, mesh.shape["depth"]), AXES
    )
    placed = (P(ROW_COL, None), P(ROW_COL, "depth"))
    return jax.shard_map(
        body, mesh=split_mesh, in_specs=placed, out_specs=P(ROW_COL, None), check_vma=False
    )
```

```python
import functools

import jax
import jax.numpy as jnp
from jax import lax
from jax.experimental import pallas as pl
from jax.experimental.pallas import tpu as pltpu
from jax.sharding import Mesh
from jax.sharding import PartitionSpec as P

W = 1024
B = 128
NBLK = W // B
PANEL = 16
AXES = ("row", "col_0", "col_1", "depth")
ROW_COL = ("row", "col_0", "col_1")
NT = (((1,), (1,)), ((), ()))
NN = (((1,), (0,)), ((), ()))
f32 = jnp.float32
bf16 = jnp.bfloat16
MESH = pl.DeviceIdType.MESH
VMEM = pl.BlockSpec(memory_space=pltpu.VMEM)


TILES = (
    (((0, 0), (1, 0), (2, 0), (3, 0)), ((4, 0), (5, 0), (6, 0), (7, 0))),
    (
        ((1, 1), (2, 1), (3, 1), (2, 2), (3, 2), (3, 3)),
        ((4, 1), (5, 1), (6, 1), (7, 1), (4, 2), (5, 2)),
    ),
    (
        ((6, 2), (7, 2), (4, 3), (5, 3), (6, 3), (7, 3), (4, 4), (5, 4)),
        ((6, 4), (7, 4), (5, 5), (6, 5), (7, 5), (6, 6), (7, 6), (7, 7)),
    ),
)
ROWS = (8, 8, 16, 24, 32)
BASE = (0, 256, 0, 1024, 2560)
STRIDE = (512, 512, 512, 768, 1024)
SOURCE = (0, 256, 0, 512, 1280)
SLOT = (0, 0, 0, 16, 40)
FAR_FIRST = (4, 3, 5, 2, 6, 1, 7)


def split(x):
    high = x.astype(bf16)
    return high, (x - high.astype(f32)).astype(bf16)


def dot3(a, b, dims=NT):
    dot = functools.partial(
        lax.dot_general, dimension_numbers=dims, preferred_element_type=f32
    )
    return dot(a[0], b[0]) + (dot(a[0], b[1]) + dot(a[1], b[0]))


def top_tiles(part, core, first, th_ref, tl_ref, a_ref, other_a_ref, tiles_ref):
    out = SOURCE[2 + part]

    def blocks(i, n=1):
        return slice(i * B, (i + n) * B)

    def value(i, j):
        if core == 1:
            return a_ref[blocks(i - 4), blocks(j)]
        if i < 4:
            return a_ref[blocks(i), blocks(j)]
        if j < 4:
            return a_ref[blocks(j), blocks(i)].T
        return other_a_ref[blocks(i - 4), blocks(j - 4)]

    todo = list(TILES[part][core])
    while todo:
        i, j = todo[0]
        n = 1
        while n < len(todo) and todo[n] == (i + n, j):
            n += 1
        todo = todo[n:]
        product = dot3(
            (th_ref[blocks(i, n), :], tl_ref[blocks(i, n), :]),
            (th_ref[blocks(j), :], tl_ref[blocks(j), :]),
        )
        for k in range(n):
            tiles_ref[out : out + B, :] = jnp.where(first, value(i + k, j), 0.0) - product[blocks(k)]
            out += B


def whole_kernel(
    past_in, a_in, out_ref,
    past_ref, a_ref, perm_ref, so_ref, u_ref, top_ref, lh_ref, ll_ref, dh_ref, dl_ref, xh_ref, xl_ref,
    to_ref, other_ref, other_a_ref, tiles_ref, ybuf, th_ref, tl_ref, part_ref, half_ref, full_ref, bun_t, bun_s,
    sc_send, sc_recv, bu_recv, fw_send, y_send, y_recv, z_send, z_recv, x_send, x_recv, d_send, d_recv,
    r_send, r_recv, g_send, g_recv, loc, swap,
):
    x = lax.axis_index("row")
    z = lax.axis_index("col_0")
    c = lax.axis_index("col_1")
    y = lax.axis_index("depth")
    me = x * 8 + z
    left = lax.rem(x + 3, 4)
    right = lax.rem(x + 1, 4)
    far = lax.rem(x + 2, 4)
    down = lax.rem(y + 3, 4)
    up = lax.rem(y + 1, 4)
    root = me == 0
    load = (
        pltpu.make_async_copy(past_in, past_ref, loc.at[5]),
        pltpu.make_async_copy(a_in, a_ref, loc.at[6]),
    )
    for copy in load:
        copy.start()
    barrier = pltpu.get_barrier_semaphore()

    def greet(*device):
        pl.semaphore_signal(barrier, inc=1, device_id=device, device_id_type=MESH)

    def z_greet(k, carry):
        greet(x, lax.rem(z + k, 8), c, y)
        return carry

    lax.fori_loop(1, 8, z_greet, 0)
    for k in range(1, 4):
        greet(x, z, c, lax.rem(y + k, 4))
    for k in range(1, 4):
        greet(lax.rem(x + k, 4), z, c, y)
    greet(x, z, 1 - c, y)

    for copy in load:
        copy.wait()
    for h in range(2):
        for q in range(32):
            to = (h * 32 + q % 8 * 4 + q // 8) * 8
            perm_ref[to : to + 8, :] = past_ref[(h * 32 + q) * 8 : (h * 32 + q) * 8 + 8, :]
    pl.semaphore_wait(barrier, 14)

    def remote(src, dst, send, recv, *device):
        return pltpu.make_async_remote_copy(
            src_ref=src, dst_ref=dst, send_sem=send, recv_sem=recv,
            device_id=device, device_id_type=MESH,
        )


    def pieces(n, core, start, count):
        at = pl.multiple_of(BASE[n] + core * STRIDE[n] + start * ROWS[n], 8)
        return (to_ref if n < 2 else so_ref).at[pl.ds(at, count * ROWS[n])]

    def slot(n, layer):
        return ybuf.at[layer, pl.ds(SLOT[n], ROWS[n])]


    def source(n, start, count):
        at = pl.multiple_of(SOURCE[n] + start * ROWS[n], 8)
        return (perm_ref if n < 2 else tiles_ref).at[pl.ds(at, count * ROWS[n])]

    def width(n):
        return 4 if n < 2 else 8

    def place_of(n, q):
        return pieces(n, c, q, 1) if n < 2 else slot(n, y)

    def bundle(n, start, count):
        ref, at = (bun_t, n * 32) if n < 2 else (bun_s, 8 * SLOT[n])
        return ref.at[pl.ds(at + start * ROWS[n], count * ROWS[n])]

    def column(n, to):
        place = (0, to) if n < 2 else (to, 0)
        src = source(n, to * width(n), width(n))
        return remote(src, bundle(n, 0, width(n)), sc_send.at[n, to], bu_recv.at[n], *place, c, y)

    def columns_all(n):
        for to in FAR_FIRST if n < 2 else (2, 1, 3):
            column(n, to).start()

    def first_piece(n, on_root, k):
        return source(n, k, 1) if on_root else bundle(n, k, 1)

    def onward(n, on_root, k):
        place = (k, z) if n < 2 else (x, k)
        dst = place_of(n, place[0] * 8 + place[1])
        return remote(first_piece(n, on_root, k), dst, fw_send.at[n, k], sc_recv.at[n], *place, c, y)

    def hub(n):
        return jnp.logical_and(x == 0 if n < 2 else z == 0, jnp.logical_not(root))

    def pass_on(n, on_root):
        own = pltpu.make_async_copy(first_piece(n, on_root, 0), place_of(n, me), loc.at[n])
        own.start()
        for k in (2, 1, 3) if n < 2 else FAR_FIRST:
            onward(n, on_root, k).start()
        own.wait()

    def stage_h(n):
        @pl.when(hub(n))
        def _():
            whole = bundle(n, 0, width(n))
            remote(whole, whole, sc_send.at[n, 0], bu_recv.at[n], 0, 0, c, y).wait_recv()
            pass_on(n, False)
            send_piece(n)

    def y_copy(n, k):
        return remote(slot(n, y), slot(n, y), y_send.at[n, k], y_recv.at[n, y], x, z, c, lax.rem(y + k, 4))

    def z_copy(n, k):
        mine = pieces(n, c, me, 1)
        return remote(mine, mine, z_send.at[n, k], z_recv.at[n, z], x, lax.rem(z + k, 8), c, y)

    def z_start(n):
        for k in FAR_FIRST:
            z_copy(n, k).start()

    def z_wait(n):
        def wait(k, carry):
            peer = lax.rem(z + k, 8)
            place = pieces(n, c, x * 8 + peer, 1)
            remote(place, place, z_send.at[n, 0], z_recv.at[n, peer], x, peer, c, y).wait_recv()
            return carry

        lax.fori_loop(1, 8, wait, 0)

    def group(n, core, g):
        return pieces(n, core, g * 8, 8)

    def half(n, g, h):
        return pieces(n, c, g * 8 + h * 4, 4)

    def x_copy(n, d):
        mine = group(n, c, x)
        return remote(mine, mine, x_send.at[n, d], x_recv.at[n, d], (right, left)[d], z, c, y)

    def x_wait(n, d):
        g = (left, right)[d]
        place = group(n, c, g)
        remote(place, place, x_send.at[n, d], x_recv.at[n, d], g, z, c, y).wait_recv()

    def relay(n, d):
        part = half(n, (left, right)[d], d)
        return remote(part, part, x_send.at[n, 2 + d], x_recv.at[n, 2 + d], (right, left)[d], z, c, y)

    def relay_wait(n, d):
        place = half(n, far, d)
        remote(place, place, x_send.at[n, 2 + d], x_recv.at[n, 2 + d], (left, right)[d], z, c, y).wait_recv()

    order = (x, left, right, far)

    def cross(n, k):
        place = group(n, c, order[k])
        return remote(place, place, d_send.at[n, k], d_recv.at[n, k], x, z, 1 - c, y)

    def send_piece(n):
        if n < 2:
            z_start(n)
        else:
            for k in range(1, 4):
                y_copy(n, k).start()

    def stage_0(n):
        columns_all(n)
        pass_on(n, True)
        send_piece(n)

    def stage_1(n):
        @pl.when(x != 0 if n < 2 else z != 0)
        def _():
            place = place_of(n, me)
            remote(place, place, sc_send.at[n, 0], sc_recv.at[n], 0, z, c, y).wait_recv()
            send_piece(n)

    def stage_y(n):
        for k in range(1, 4):
            peer = lax.rem(y + k, 4)
            place = slot(n, peer)
            remote(place, place, y_send.at[n, 0], y_recv.at[n, peer], x, z, c, peer).wait_recv()
        rows = slice(SLOT[n], SLOT[n] + ROWS[n])
        at = pl.multiple_of(BASE[n] + c * STRIDE[n] + me * ROWS[n], 8)
        so_ref[pl.ds(at, ROWS[n]), :] = (ybuf[0, rows] + ybuf[1, rows]) + (ybuf[2, rows] + ybuf[3, rows])
        z_start(n)

    def stage_2(n):
        z_wait(n)
        cross(n, 0).start()
        for d in range(2):
            x_copy(n, d).start()

    def stage_3(n):
        for d in range(2):
            x_wait(n, d)
            cross(n, 1 + d).start()
            relay(n, d).start()

    def stage_4(n):
        for d in range(2):
            relay_wait(n, d)
        cross(n, 3).start()

    def stage_5(n):
        for k in range(4):
            place = group(n, 1 - c, order[k])
            remote(place, place, d_send.at[n, k], d_recv.at[n, k], x, z, 1 - c, y).wait_recv()


    def update(h):
        for n in range(2):
            at = slice(n * 512 + h * 256, n * 512 + h * 256 + 256)
            th_ref[at, :], tl_ref[at, :] = split(to_ref[at, :])
        for k in (2, 1, 3, 0):
            at = pl.multiple_of(lax.rem(y + k, 4) * B, B)
            mine = split(past_ref[pl.ds(at, B), :])
            for n in range(2):
                top = slice(n * 512 + h * 256, n * 512 + h * 256 + 256)
                part_ref[k, h, :, n * 256 : n * 256 + 256] = dot3(mine, (th_ref[top, :], tl_ref[top, :]))
            if k == 2:
                for d in range(2):
                    reduce_first(h, d).start()
            elif k:
                reduce_own(h, k // 2).start()

    def reduce_first(h, d):
        return remote(
            part_ref.at[2, h, pl.ds(d * 64, 64)], half_ref.at[h, d], r_send.at[h, d], r_recv.at[h, d],
            x, z, c, (up, down)[d],
        )

    def reduce_own(h, d):
        rows = pl.ds(64 - d * 64, 64)
        return remote(
            part_ref.at[1 + 2 * d, h, rows], full_ref.at[h, d, rows], r_send.at[h, 2 + d], r_recv.at[h, 2 + d],
            x, z, c, (up, down)[d],
        )

    def reduce_sum(h, d):
        rows = pl.ds(d * 64, 64)
        return remote(
            part_ref.at[1 + 2 * d, h, rows], full_ref.at[h, d, rows], r_send.at[h, 4 + d], r_recv.at[h, 4 + d],
            x, z, c, (up, down)[d],
        )

    def update_2(h):
        for d in range(2):
            reduce_first(h, d).wait_recv()
            rows = slice(d * 64, d * 64 + 64)
            part_ref[1 + 2 * d, h, rows, :] += half_ref[h, d]
            reduce_sum(h, d).start()

    def gather(h, d):
        to = pl.ds((1 + 2 * d) * B, B)
        return remote(
            u_ref.at[h, pl.ds(0, B)], u_ref.at[h, to], g_send.at[h, d], g_recv.at[h, d], x, z, c, (up, down)[d]
        )

    def gather_on(h, d):
        mine = pl.ds((1 + 2 * d) * B + d * 64, 64)
        to = pl.ds(2 * B + d * 64, 64)
        return remote(
            u_ref.at[h, mine], u_ref.at[h, to], g_send.at[h, 2 + d], g_recv.at[h, 2 + d], x, z, c, (up, down)[d]
        )

    def update_3(h):
        for d in range(2):
            reduce_own(h, d).wait_recv()
            reduce_sum(h, d).wait_recv()
        at = pl.multiple_of(y * B, B)
        for n in range(2):
            cols = slice(n * 256, n * 256 + 256)
            mat = a_ref[pl.ds(at, B), n * 512 + h * 256 : n * 512 + h * 256 + 256]
            u_ref[h, 0:B, cols] = mat - (part_ref[0, h, :, cols] + (full_ref[h, 0, :, cols] + full_ref[h, 1, :, cols]))
        for d in range(2):
            gather(h, d).start()

    def update_4(h):
        for d in range(2):
            gather(h, d).wait_recv()
            gather_on(h, d).start()

    def update_5(h):
        for d in range(2):
            gather_on(h, d).wait_recv()

    def take(part):
        for core in range(2):
            at = BASE[2 + part] + core * STRIDE[2 + part]
            for n, (i, j) in enumerate(TILES[part][core]):
                top_ref[i * B : i * B + B, j * B : j * B + B] += so_ref[at + n * B : at + n * B + B, :]


    trade = remote(past_ref, other_ref, swap.at[0], swap.at[1], x, z, 1 - c, y)
    trade_a = remote(a_ref.at[:, pl.ds(512, 512)], other_a_ref, swap.at[2], swap.at[3], x, z, 1 - c, y)

    @pl.when(root)
    def _():
        trade.start()
        trade_a.start()
        stage_0(0)
        stage_0(1)
        mine = pl.ds(pl.multiple_of(c * 512, 512), 512)
        theirs = pl.ds(pl.multiple_of(512 - c * 512, 512), 512)
        th_ref[mine, :], tl_ref[mine, :] = split(past_ref[...])
        trade.wait_recv()
        th_ref[theirs, :], tl_ref[theirs, :] = split(other_ref[...])
        trade_a.wait_recv()
        for part in range(3):
            for core in range(2):
                @pl.when(c == core)
                def _(part=part, core=core):
                    top_tiles(part, core, y == 0, th_ref, tl_ref, a_ref, other_a_ref, tiles_ref)

        stage_0(2)

    rows_0, rows_1, tiles_a, tiles_b, tiles_c = range(5)

    for i in range(NBLK):
        top_ref[i * B : i * B + B, 0 : i * B + B] = jnp.zeros((B, i * B + B), f32)

    def next_part(n):
        @pl.when(root)
        def _():
            stage_0(n)

    def next_part(n):
        @pl.when(root)
        def _():
            stage_0(n)

    stage_h(rows_0)
    stage_1(rows_0)
    stage_h(tiles_a)
    stage_h(rows_1)
    stage_2(rows_0)
    next_part(tiles_b)
    stage_1(rows_1)
    stage_1(tiles_a)
    stage_3(rows_0)
    stage_y(tiles_a)
    stage_4(rows_0)
    stage_h(tiles_b)
    stage_2(rows_1)
    next_part(tiles_c)
    stage_1(tiles_b)
    stage_5(rows_0)
    stage_h(tiles_c)
    stage_2(tiles_a)
    stage_3(rows_1)
    stage_y(tiles_b)
    update(0)
    stage_3(tiles_a)
    stage_4(rows_1)
    stage_1(tiles_c)
    stage_2(tiles_b)
    stage_4(tiles_a)
    update_2(0)
    stage_5(rows_1)
    stage_y(tiles_c)
    update(1)
    stage_3(tiles_b)
    stage_5(tiles_a)
    take(0)

    def stage_5b():
        stage_5(tiles_b)
        take(1)

    def stage_5c():
        stage_5(tiles_c)
        take(2)

    finish = functools.partial(
        solve, y, u_ref, lh_ref, ll_ref, dh_ref, dl_ref, out_ref, xh_ref, xl_ref
    )

    def update_5ab():
        update_5(0)
        update_5(1)

    events = {
        (0, 4): lambda: stage_4(tiles_b),
        (0, 5): lambda: stage_2(tiles_c),
        (0, 6): lambda: update_2(1),
        (0, 7): lambda: update_3(0),
        (1, -1): stage_5b,
        (1, 6): lambda: stage_3(tiles_c),
        (2, 2): lambda: update_3(1),
        (2, 6): lambda: stage_4(tiles_c),
        (3, 2): stage_5c,
        (3, 3): lambda: update_4(0),
        (5, 1): lambda: update_4(1),
        (6, 6): update_5ab,
        (7, 0): lambda: finish(0),
        (7, 2): lambda: finish(1),
        (7, 4): lambda: finish(2),
    }
    factor_top(lh_ref, ll_ref, dh_ref, dl_ref, top_ref, events)
    finish(3)


    @pl.when(root)
    def _():
        trade.wait_send()
        trade_a.wait_send()

        for n in range(5):
            for to in range(1, 8 if n < 2 else 4):
                column(n, to).wait_send()
            for k in range(1, width(n)):
                onward(n, True, k).wait_send()

    for n in range(5):
        @pl.when(hub(n))
        def _(n=n):
            for k in range(1, width(n)):
                onward(n, False, k).wait_send()

    def done_z(k, carry):
        for n in range(5):
            z_copy(n, k).wait_send()
        return carry

    lax.fori_loop(1, 8, done_z, 0)
    for n in range(5):
        if n >= 2:
            for k in range(1, 4):
                y_copy(n, k).wait_send()
        for d in range(2):
            x_copy(n, d).wait_send()
            relay(n, d).wait_send()
        for k in range(4):
            cross(n, k).wait_send()
    for h in range(2):
        for d in range(2):
            reduce_first(h, d).wait_send()
            reduce_own(h, d).wait_send()
            reduce_sum(h, d).wait_send()
            gather(h, d).wait_send()
            gather_on(h, d).wait_send()


def inverse_factor(w, fill):
    lane = lax.broadcasted_iota(jnp.int32, (B, B), 1)
    sub = lax.broadcasted_iota(jnp.int32, (B, B), 0)
    k = PANEL
    at = sub[:k]
    done = []
    for t in range(B // k):
        r0 = t * k
        left = B - r0
        cols = [jnp.broadcast_to(w[:, r0 + m : r0 + m + 1], (left, B)) for m in range(k)]
        lanes, subs = lane[:left], sub[:left]
        unit = jnp.where((lanes == subs + r0) & (subs < k), 1.0, 0.0)
        w = jnp.where((lanes >= r0) & (lanes < r0 + k), unit, w)
        rows = w[:k]
        piv = jnp.stack([col[:k] for col in cols])
        final = jnp.zeros((k, B), f32)
        for m in range(k):
            mine, rest = piv[0], piv[1:]
            inv = lax.rsqrt(jnp.broadcast_to(mine[m : m + 1], (k, B)))
            inv2 = inv * inv
            row = jnp.broadcast_to(rows[m : m + 1], (k, B))
            here = at == m
            final = jnp.where(here, row * inv, final)
            step = row * inv2
            rows = jnp.where(here, step, rows - mine * step)
            if m + 1 < k:
                f = jnp.broadcast_to(rest[:, m : m + 1], (k - 1 - m, k, B)) * inv2[None]
                piv = jnp.where(here[None], f, rest - mine[None] * f)
        done.append(jnp.where(lane[:k] <= at + r0, final, 0.0))
        if left > k:
            w = w[k:]
            for m in range(k):
                w = w - cols[m][k:] * jnp.broadcast_to(rows[m : m + 1], (left - k, B))
        fill(t)
    return jnp.concatenate(done, axis=0)


def factor_top(lh_ref, ll_ref, dh_ref, dl_ref, a_ref, events):
    def rows(i, n=1):
        return slice(i * B, (i + n) * B)

    def low(i, n, j):
        return lh_ref[rows(i, n), rows(j)], ll_ref[rows(i, n), rows(j)]

    def panel(i, n, s, d):
        high, lo = split(dot3(split(a_ref[rows(i, n), rows(s)]), d))
        lh_ref[rows(i, n), rows(s)] = high
        ll_ref[rows(i, n), rows(s)] = lo

    def trail(i, n, j, nj, s):
        a_ref[rows(i, n), rows(j, nj)] -= dot3(low(i, n, s), low(j, nj, s))

    waiting = []
    halves = [None, None]
    for s in range(NBLK):
        def fill(t, s=s):
            if (s, t) in events:
                events[s, t]()
            if s == 3 and t < 2:
                return
            n = -(-len(waiting) // (B // PANEL - t))
            for _ in range(n):
                waiting.pop(0)()

        if (s, -1) in events:
            events[s, -1]()
        d = split(inverse_factor(a_ref[rows(s), rows(s)], fill))
        halves[s % 2] = d
        at = (s % 2) * B
        dh_ref[s // 2, at : at + B, at : at + B] = d[0]
        dl_ref[s // 2, at : at + B, at : at + B] = d[1]
        if s % 2 == 0:
            dh_ref[s // 2, 0:B, B : 2 * B] = jnp.zeros((B, B), bf16)
            dl_ref[s // 2, 0:B, B : 2 * B] = jnp.zeros((B, B), bf16)
        if s + 1 < NBLK:
            panel(s + 1, 1, s, d)
            trail(s + 1, 1, s + 1, 1, s)
        if s + 2 < NBLK:
            def rest(s=s, d=d):
                panel(s + 2, NBLK - s - 2, s, d)

            waiting.append(rest)
            waiting.append(functools.partial(trail, s + 2, NBLK - s - 2, s + 1, 1, s))
            for j in range(s + 2, NBLK):
                waiting.append(functools.partial(trail, j, NBLK - j, j, 1, s))
        if s % 2 == 1:
            def corner(s=s, first=halves[0], second=halves[1]):
                mid = dot3(low(s, 1, s - 1), first, NN)
                high, lo = split(-dot3(second, split(mid), NN))
                dh_ref[s // 2, B : 2 * B, 0:B] = high
                dl_ref[s // 2, B : 2 * B, 0:B] = lo

            waiting.append(corner)
    for job in waiting:
        job()


def solve(depth, u_ref, lh_ref, ll_ref, dh_ref, dl_ref, out_ref, xh, xl, n):
    cols = slice(n * 256, n * 256 + 256)
    u = u_ref[n % 2, :, (n // 2) * 256 : (n // 2) * 256 + 256]
    if n:
        done = slice(0, n * 256)
        u = u - dot3((xh[:, done], xl[:, done]), (lh_ref[cols, done], ll_ref[cols, done]))
    out = dot3(split(u), (dh_ref[n], dl_ref[n]))
    if n < 3:
        xh[:, cols], xl[:, cols] = split(out)
    for q in range(4):
        place = pl.multiple_of(lax.rem(depth + 4 - q, 4) * B, B)
        out_ref[pl.ds(place, B), cols] = out[q * B : q * B + B, :]


def body(a_cols, past):
    dma = pltpu.SemaphoreType.DMA
    vmem = pltpu.VMEM
    solved = pl.pallas_call(
        whole_kernel,
        out_shape=jax.ShapeDtypeStruct((512, W), f32),
        in_specs=[pl.BlockSpec(memory_space=pltpu.HBM)] * 2,
        out_specs=VMEM,
        scratch_shapes=[
            vmem((512, 512), f32),
            vmem((512, W), f32),
            vmem((512, 512), f32),
            vmem((36 * B, B), f32),
            vmem((2, 4 * B, 512), f32),
            vmem((W, W), f32),
            vmem((W, W), bf16),
            vmem((W, W), bf16),
            vmem((4, 256, 256), bf16),
            vmem((4, 256, 256), bf16),
            vmem((4 * B, W), bf16),
            vmem((4 * B, W), bf16),
            vmem((W, 512), f32),
            vmem((512, 512), f32),
            vmem((512, 512), f32),
            vmem((18 * B, B), f32),
            vmem((4, 72, B), f32),
            vmem((W, 512), bf16),
            vmem((W, 512), bf16),
            vmem((4, 2, B, 512), f32),
            vmem((2, 2, 64, 512), f32),
            vmem((2, 2, B, 512), f32),
            vmem((64, 512), f32),
            vmem((576, B), f32),
            dma((5, 8)), dma((5,)), dma((5,)), dma((5, 8)), dma((5, 4)), dma((5, 4)), dma((5, 8)), dma((5, 8)),
            dma((5, 4)), dma((5, 4)), dma((5, 4)), dma((5, 4)),
            dma((2, 6)), dma((2, 6)), dma((2, 4)), dma((2, 4)), dma((7,)), dma((4,)),
        ],
        compiler_params=pltpu.CompilerParams(collective_id=0, has_side_effects=True, vmem_limit_bytes=40 * 2**20),
        name="whole",
    )(past, a_cols)
    x, z, c = (lax.axis_index(axis) for axis in ROW_COL)
    row = (x * 16 + z * 2 + c) * 512 + lax.broadcasted_iota(jnp.int32, (512, W), 0)
    return jnp.where(row >= lax.broadcasted_iota(jnp.int32, (512, W), 1), solved, 0.0)


def solution(mesh):
    split_mesh = Mesh(
        mesh.devices.reshape(mesh.shape["row"], 8, 2, mesh.shape["depth"]), AXES
    )
    placed = (P(ROW_COL, None), P(ROW_COL, "depth"))
    return jax.shard_map(
        body, mesh=split_mesh, in_specs=placed, out_specs=P(ROW_COL, None), check_vma=False
    )
```
